32 devices in a mesh: rep: 2 (over x), exp: 4 (over z), ten: 4 (over y, core).
Axes of the slice: x: 2, y: 2, z: 4, core: 2. Of those that a mesh axis runs over, the one named last changes fastest.
Arguments:
- hidden_in: bfloat16 [768, 3072], P(('rep', 'exp', 'ten')), parts along dimension 0, may hold values from -6 to 6
- queries: bfloat16 [768, 6144], P(('rep', 'exp', 'ten')), parts along dimension 0, may hold values from -100 to 100
- new_kv: bfloat16 [2, 768, 1024], P(None, ('rep', 'exp', 'ten')), parts along dimension 1, may hold values from -5 to 5
- prefix_kv: bfloat16 [2, 8, 128, 1024], P(None, ('rep', 'exp'), 'ten'), parts along dimension 1, may hold values from -5 to 5
- decode_kv: bfloat16 [2, 128, 48, 1024], P(None, ('rep', 'exp', 'ten')), parts along dimension 1, may hold values from -5 to 5
- prefix_len: int32 [8], P(('rep', 'exp')), parts along dimension 0, may hold values from 2 to 128
- decode_len: int32 [128], P(('rep', 'exp', 'ten')), parts along dimension 0, may hold values from 2 to 48
- out_proj: bfloat16 [6144, 3072], P('ten'), may hold values from -0.078125 to 0.078125
- norm_gain: float32 [3072], replicated, may hold values from 0.5 to 1.5
- router_w: bfloat16 [3072, 8], replicated, may hold values from -0.109375 to 0.109375
- expert_ids: int32 [768, 2], P(('rep', 'exp', 'ten')), parts along dimension 0, may hold values from 0 to 7, all different within a row; in each aligned block of 24 rows (0 to 23, 24 to 47, ...) at most 7 rows name the same one
- w_gate: bfloat16 [8, 3072, 8192], P('exp', None, 'ten'), may hold values from -0.109375 to 0.109375
- w_up: bfloat16 [8, 3072, 8192], P('exp', None, 'ten'), may hold values from -0.109375 to 0.109375
- w_down: bfloat16 [8, 8192, 3072], P('exp', 'ten'), may hold values from -0.0625 to 0.0625
Outputs:
- layer_out: bfloat16 [768, 3072], P(('rep', 'exp', 'ten')), parts along dimension 0
The draws below stay inside these ranges and needn't reach their ends.
There are 2 independent parts, one for each index of `rep`. The reference program is written for one: setup_inputs(seed, part) draws one part's arguments, and reference() takes and returns one part's arrays. A program takes and returns all parts, laid end to end along the dimension named above; an argument that names none is the same for every part. Nothing has to cross between parts.
Inputs may be any that keep to these rules, and one draw needn't show every extreme that they name: `expert_ids`: each row names two different experts. Within each aligned block of 24 rows (the rows of one device) no expert is named by more than 7 rows, and in some block one expert is named by exactly 7 rows.
All inputs are finite; a program needn't handle non-finite values.
Results may differ from the reference program's by a relative error of at most 0.013.
Values may be sent and summed in bfloat16 or wider, within the bound.
No kernel may reach another device: no remote copies, remote signals or barrier semaphores. Data moves between devices by JAX's collectives and lax.ppermute only.
A program may use at most 128 MiB of HBM per device.

```python
import math
import jax
import jax.numpy as jnp
import numpy as np
from jax import lax

D = 3072
FF = 8192
HQ = 48
KVH = 8
HD = 128
EXPERTS = 8
ROWS_DEV = 24
DEC_DEV = 4
CTX_DEC = 48
CAP = 7
CH_DEV = 20
GROUP_ROWS = 96
SPAN = 80
DEC_GROUP = 16
TOKENS = 384
PREFIX = 128
DEC_ALL = 64
N_EXP = 4
N_TEN = 4


def joint_fields(key):
    base_key = jax.random.fold_in(key, 4417)
    key_query, key_prefix, key_decode = jax.random.split(base_key, 3)
    query_field = jnp.clip(jax.random.normal(key_query, (N_EXP, GROUP_ROWS, HQ, HD), jnp.float32), -5.0, 5.0)
    prefix_field = jnp.clip(jax.random.normal(key_prefix, (2, N_EXP, PREFIX, KVH, HD), jnp.float32), -5.0, 5.0)
    decode_field = jnp.clip(jax.random.normal(key_decode, (2, DEC_ALL, CTX_DEC, KVH, HD), jnp.float32), -5.0, 5.0)
    return (query_field, prefix_field, decode_field)


def draw_queries(key, part):
    return joint_fields(key)[0].reshape(TOKENS, HQ * HD).astype(jnp.bfloat16)


def draw_prefix_kv(key, part):
    return joint_fields(key)[1].reshape(2, N_EXP, PREFIX, KVH * HD).astype(jnp.bfloat16)


def draw_decode_kv(key, part):
    return joint_fields(key)[2].reshape(2, DEC_ALL, CTX_DEC, KVH * HD).astype(jnp.bfloat16)


def plant(entries, key, smallest, high):
    spot = [jax.random.randint(jax.random.fold_in(key, axis), (), 0, length) for axis, length in enumerate(entries.shape)]
    main_axis = entries.shape.index(max(entries.shape))
    neighbour = spot[:main_axis] + [(spot[main_axis] + 1) % entries.shape[main_axis]] + spot[main_axis + 1:]
    return entries.at[tuple(spot)].set(smallest).at[tuple(neighbour)].set(high)


def block_scale(stream_key, dims, cuts, smallest, top_value):
    factor_of = 1.0
    for position, blocks in cuts:
        steps = jax.random.uniform(jax.random.fold_in(jax.random.fold_in(stream_key, 6), position), (blocks,), jnp.float32, smallest / len(cuts), top_value / len(cuts))
        factor_of = factor_of * jnp.repeat(jnp.exp(steps), dims[position] // blocks).reshape((-1,) + (1,) * (len(dims) - 1 - position))
    return factor_of


def deal_out(key, own, number, rows, number_of, top, reach, skew):
    sequence = jax.random.permutation(key, number_of)
    packed, usual = load_shares(number_of, rows * top, reach, skew, True), load_shares(number_of, rows * top, reach, skew, False)
    places = jnp.arange(number_of)

    def named(sizes, offset_by):
        used = int((sizes > 0).sum())
        fixed = max(1, used // 4)
        shifted = fixed + (places - fixed + offset_by * (used - fixed)) % max(1, number_of - fixed)
        return jnp.zeros((number_of,), jnp.int32).at[sequence[jnp.where(places < fixed, places, shifted)]].set(jnp.asarray(sizes, jnp.int32))

    sizes = jnp.where(number % 4 == 0, named(packed, number // 4), named(usual, number - number // 4 - 1))
    mixed = jax.random.permutation(jax.random.fold_in(own, 3), number_of)
    giver, receiver = mixed[0:number_of // 2 * 2:2], mixed[1:number_of // 2 * 2:2]
    slack = jnp.minimum(sizes[giver] - 1, reach - sizes[receiver]) // 2
    slack = jnp.where((giver == sequence[0]) | (receiver == sequence[0]) | (sizes[receiver] == 0), 0, jnp.maximum(slack, 0))
    shifted = jax.random.randint(jax.random.fold_in(own, 4), (number_of // 2,), 0, 1 << 20) % (slack + 1)
    sizes = sizes.at[giver].add(-shifted).at[receiver].add(shifted)
    items = jnp.searchsorted(jnp.cumsum(sizes), jnp.arange(rows * top), side="right").astype(jnp.int32)
    grid = items.reshape(top, rows).T
    grid = grid[jax.random.permutation(jax.random.fold_in(own, 1), rows)]
    offset_by = jax.random.randint(jax.random.fold_in(own, 2), (rows, 1), 0, top)
    return jnp.take_along_axis(grid, (jnp.arange(top)[None, :] + offset_by) % top, axis=1)


def load_shares(number_of, total, reach, slope, full):
    portions = [(1 << 20) // math.isqrt(grade ** slope) + 1 for grade in range(1, number_of + 1)]
    largest = reach if full else min(reach, max(-(-total // number_of), total * portions[0] // sum(portions)))
    least = 1 if total - largest >= number_of - 1 else 0
    given, surplus = [largest] + [least] * (number_of - 1), total - largest - least * (number_of - 1)
    while surplus > 0:
        free = [i for i in range(1, number_of) if given[i] < largest] or [i for i in range(1, number_of) if given[i] < reach]
        whole, left = sum([portions[i] for i in free]), surplus
        for i in free:
            more = min(reach - given[i], max(1, left * portions[i] // whole), surplus)
            given[i] = given[i] + more
            surplus = surplus - more
    return np.array(given)


def noise(stream_key, shape, deviation, bound, shards=(), kind=jnp.bfloat16):
    loudness = block_scale(stream_key, shape, shards, -0.22, 0.18) if shards else 1.0
    entries = jax.random.normal(stream_key, shape, jnp.float32) * deviation * loudness
    return jnp.minimum(jnp.maximum(entries, -bound), bound).astype(kind)


def setup_inputs(seed: int = 0, part: int = 0) -> dict:
    splits = jax.random.split(jax.random.key(seed), 15)
    part_keys = jax.random.split(jax.random.fold_in(splits[14], part), 15)
    hidden_in = noise(part_keys[0], (TOKENS, D), 1.0, 6.0, ((0, 16),))
    queries = draw_queries(jax.random.fold_in(jax.random.fold_in(splits[14], part), 71), part)
    new_kv = noise(part_keys[2], (2, TOKENS, KVH * HD), 1.0, 5.0, ((1, 16),))
    prefix_kv = draw_prefix_kv(jax.random.fold_in(jax.random.fold_in(splits[14], part), 71), part)
    decode_kv = draw_decode_kv(jax.random.fold_in(jax.random.fold_in(splits[14], part), 71), part)
    prefix_len = plant(jax.random.randint(part_keys[5], (N_EXP,), 2, PREFIX + 1), jax.random.fold_in(part_keys[5], 1), 2, PREFIX).astype(jnp.int32)
    decode_len = plant(jax.random.randint(part_keys[6], (DEC_ALL,), 2, CTX_DEC + 1), jax.random.fold_in(part_keys[6], 1), 2, CTX_DEC).astype(jnp.int32)
    out_proj = noise(splits[7], (HQ * HD, D), (HQ * HD) ** -0.5, 0.078125, ((0, 4),))
    norm_gain = jnp.clip(1.0 + 0.1 * jax.random.normal(splits[8], (D,), jnp.float32), 0.5, 1.5)
    router_w = noise(splits[9], (D, EXPERTS), D ** -0.5, 0.109375)
    expert_ids_keys = jax.random.split(jax.random.fold_in(part_keys[10], 1), TOKENS // ROWS_DEV)
    expert_ids_turns = jax.random.permutation(jax.random.fold_in(part_keys[10], 3), TOKENS // ROWS_DEV)
    expert_ids = jax.vmap(lambda own, number: deal_out(jax.random.fold_in(part_keys[10], 2), own, number, ROWS_DEV, EXPERTS, 2, CAP, 2))(expert_ids_keys, expert_ids_turns).reshape((TOKENS, 2))
    w_gate = noise(splits[11], (EXPERTS, D, FF), D ** -0.5, 0.109375, ((0, 4), (2, 4)))
    w_up = noise(splits[12], (EXPERTS, D, FF), D ** -0.5, 0.109375, ((0, 4), (2, 4)))
    w_down = noise(splits[13], (EXPERTS, FF, D), FF ** -0.5, 0.0625, ((0, 4), (1, 4)))
    return {"hidden_in": hidden_in, "queries": queries, "new_kv": new_kv, "prefix_kv": prefix_kv, "decode_kv": decode_kv, "prefix_len": prefix_len, "decode_len": decode_len, "out_proj": out_proj, "norm_gain": norm_gain, "router_w": router_w, "expert_ids": expert_ids, "w_gate": w_gate, "w_up": w_up, "w_down": w_down}


def attend(scores, visible, values, pattern):
    masked = jnp.where(visible, scores, -jnp.inf)
    row_max = lax.optimization_barrier(jnp.max(masked, axis=-1, keepdims=True))
    exponent = jnp.exp(masked - row_max)
    totals = lax.optimization_barrier(jnp.sum(exponent, axis=-1))
    weights = exponent.astype(jnp.bfloat16).astype(jnp.float32)
    return (jnp.einsum(pattern, weights, values) / totals[..., None]).astype(jnp.bfloat16)

def group_attention(group, queries, new_kv, prefix_kv, decode_kv, prefix_len, decode_len):
    per_kv = HQ // KVH
    score_scale = HD ** (-0.5)
    first_row = group * GROUP_ROWS
    query_rows = queries[first_row:first_row + GROUP_ROWS].astype(jnp.float32).reshape(N_TEN, ROWS_DEV, KVH, per_kv, HD)
    key_rows = new_kv[0, first_row:first_row + GROUP_ROWS].astype(jnp.float32).reshape(N_TEN, ROWS_DEV, KVH, HD)
    value_rows = new_kv[1, first_row:first_row + GROUP_ROWS].astype(jnp.float32).reshape(N_TEN, ROWS_DEV, KVH, HD)
    span_queries = query_rows[:, :CH_DEV].reshape(SPAN, KVH, per_kv, HD)
    span_keys = key_rows[:, :CH_DEV].reshape(SPAN, KVH, HD)
    span_values = value_rows[:, :CH_DEV].reshape(SPAN, KVH, HD)
    prefill_keys = jnp.concatenate([prefix_kv[0, group].astype(jnp.float32).reshape(PREFIX, KVH, HD), span_keys], axis=0)
    prefill_values = jnp.concatenate([prefix_kv[1, group].astype(jnp.float32).reshape(PREFIX, KVH, HD), span_values], axis=0)
    scores = jnp.einsum('rcgh,pch->rcgp', span_queries, prefill_keys) * score_scale
    positions = jnp.arange(PREFIX + SPAN, dtype=jnp.int32)[None, :]
    row_index = jnp.arange(SPAN, dtype=jnp.int32)[:, None]
    visible = jnp.where(positions < PREFIX, positions < prefix_len[group], positions - PREFIX <= row_index)
    prefill_out = attend(scores, visible[:, None, None, :], prefill_values, 'rcgp,pch->rcgh')
    first_seq = group * DEC_GROUP
    dec_queries = query_rows[:, CH_DEV:].reshape(DEC_GROUP, KVH, per_kv, HD)
    own_keys = key_rows[:, CH_DEV:].reshape(DEC_GROUP, KVH, HD)
    own_values = value_rows[:, CH_DEV:].reshape(DEC_GROUP, KVH, HD)
    decode_keys = jnp.concatenate([decode_kv[0, first_seq:first_seq + DEC_GROUP].astype(jnp.float32).reshape(DEC_GROUP, CTX_DEC, KVH, HD), own_keys[:, None]], axis=1)
    decode_values = jnp.concatenate([decode_kv[1, first_seq:first_seq + DEC_GROUP].astype(jnp.float32).reshape(DEC_GROUP, CTX_DEC, KVH, HD), own_values[:, None]], axis=1)
    decode_scores = jnp.einsum('dcgh,dpch->dcgp', dec_queries, decode_keys) * score_scale
    decode_pos = jnp.arange(CTX_DEC + 1, dtype=jnp.int32)[None, :]
    lengths = decode_len[first_seq:first_seq + DEC_GROUP][:, None]
    visible_dec = (decode_pos < lengths) | (decode_pos == CTX_DEC)
    decode_out = attend(decode_scores, visible_dec[:, None, None, :], decode_values, 'dcgp,dpch->dcgh')
    combined = jnp.concatenate([prefill_out.reshape(N_TEN, CH_DEV, HQ * HD), decode_out.reshape(N_TEN, DEC_DEV, HQ * HD)], axis=1)
    return combined.reshape(GROUP_ROWS, HQ * HD)

def run_expert(bundle):
    slot_rows, gate_weight, up_weight, down_weight = bundle
    gate_act = jnp.dot(slot_rows, gate_weight, preferred_element_type=jnp.float32)
    up_act = jnp.dot(slot_rows, up_weight, preferred_element_type=jnp.float32)
    hidden = (jax.nn.silu(gate_act) * up_act).astype(jnp.bfloat16)
    return jnp.dot(hidden, down_weight, preferred_element_type=jnp.float32).astype(jnp.bfloat16)

def reference(hidden_in, queries, new_kv, prefix_kv, decode_kv, prefix_len, decode_len, out_proj, norm_gain, router_w, expert_ids, w_gate, w_up, w_down):
    pieces = []
    for group in range(N_EXP):
        pieces.append(group_attention(group, queries, new_kv, prefix_kv, decode_kv, prefix_len, decode_len))
    attended = jnp.concatenate(pieces, axis=0)
    residual = hidden_in.astype(jnp.float32) + jnp.dot(attended, out_proj, preferred_element_type=jnp.float32)
    mean_square = lax.optimization_barrier(jnp.mean(residual * residual, axis=1, keepdims=True))
    normed = (residual * lax.rsqrt(mean_square + 1e-05) * norm_gain).astype(jnp.bfloat16)
    logits = jnp.dot(normed, router_w, preferred_element_type=jnp.float32)
    chosen_logits = jnp.take_along_axis(logits, expert_ids, axis=1)
    route_weights = jax.nn.softmax(chosen_logits, axis=1)
    blocks = TOKENS // ROWS_DEV
    chosen = expert_ids.reshape(blocks, ROWS_DEV * 2)
    chosen_hot = (chosen[:, :, None] == jnp.arange(EXPERTS, dtype=jnp.int32)).astype(jnp.int32)
    earlier = jnp.cumsum(chosen_hot, axis=1) - chosen_hot
    slot_rank = lax.optimization_barrier(jnp.sum(earlier * chosen_hot, axis=2))
    slot_flat = (jnp.arange(blocks, dtype=jnp.int32)[:, None] * CAP + slot_rank).reshape(-1).astype(jnp.int32)
    expert_flat = expert_ids.reshape(-1).astype(jnp.int32)
    token_of = jnp.repeat(jnp.arange(TOKENS, dtype=jnp.int32), 2)
    buffer = jnp.zeros((EXPERTS, blocks * CAP, D), jnp.bfloat16).at[expert_flat, slot_flat].set(normed[token_of])
    expert_out = lax.map(run_expert, (buffer, w_gate, w_up, w_down))
    picked = expert_out[expert_flat, slot_flat].reshape(TOKENS, 2, D).astype(jnp.float32)
    mixed = residual + route_weights[:, 0:1] * picked[:, 0] + route_weights[:, 1:2] * picked[:, 1]
    return mixed.astype(jnp.bfloat16)
```

```python
import functools

import jax
import jax.numpy as jnp
from jax import lax
from jax.experimental import pallas as pl
from jax.experimental.pallas import tpu as pltpu
from jax.sharding import PartitionSpec as P

HD = 128
SLOTS = 8
F32 = jnp.float32
BF16 = jnp.bfloat16
VMEM = pl.BlockSpec(memory_space=pltpu.VMEM)
SMEM = pl.BlockSpec(memory_space=pltpu.SMEM)
ANY = pl.BlockSpec(memory_space=pl.ANY)


def xor_pairs(size, distance):
    return [(i, i ^ distance) for i in range(size)]


def bit_reversed(size):
    order = [0]
    step = size // 2
    while step:
        order = order + [o + step for o in order]
        step //= 2
    return order


def up_bits(size):
    return [1 << b for b in range(size.bit_length() - 1)]


def pack_kernel(q_ref, new_ref, prefix_ref, *out_refs, heads_own, per_kv, kv_own):
    me = lax.axis_index("ten")
    rows = q_ref.shape[0]
    prefix_rows = prefix_ref.shape[2]
    width = kv_own * HD
    pieces = heads_own // kv_own
    for d, out in enumerate(out_refs):
        t = me ^ d
        q_start = pl.multiple_of(t * (heads_own * HD), HD)
        for j in range(pieces):
            out[j * rows : (j + 1) * rows, :] = q_ref[
                :, pl.ds(pl.multiple_of(q_start + j * width, HD), width)
            ]
        kv_start = pl.multiple_of(((t * heads_own) // per_kv) * HD, HD)
        base = pieces * rows
        for s in range(2):
            out[base : base + rows, :] = new_ref[s, :, pl.ds(kv_start, width)]
            base += rows
        for s in range(2):
            out[base : base + prefix_rows, :] = prefix_ref[s, 0, :, pl.ds(kv_start, width)]
            base += prefix_rows


def decode_kernel(len_ref, q_ref, kv_ref, new_ref, *refs, per_kv, span_dev):
    out_refs, scratch = refs[:-1], refs[-1]
    me = lax.axis_index("ten")
    dec_dev, ctx_len, kv_width = kv_ref.shape[1:]
    heads = q_ref.shape[0] // dec_dev
    heads_kv = kv_width // HD
    scale = HD ** (-0.5)
    row_group = lax.broadcasted_iota(jnp.int32, (heads, kv_width), 0) // per_kv
    lane_group = lax.broadcasted_iota(jnp.int32, (heads, kv_width), 1) // HD
    own = row_group == lane_group
    position = lax.broadcasted_iota(jnp.int32, (heads, ctx_len), 1)
    for r in range(dec_dev):
        q = q_ref[r * heads : (r + 1) * heads, :]
        wide = jnp.where(own, jnp.concatenate([q] * heads_kv, axis=1), jnp.zeros((), BF16))
        scores = (
            lax.dot_general(
                wide, kv_ref[0, r], (((1,), (1,)), ((), ())), preferred_element_type=F32
            )
            * scale
        )
        new_key = new_ref[0, span_dev + r : span_dev + r + 1, :].astype(F32)
        new_value = new_ref[1, span_dev + r : span_dev + r + 1, :].astype(F32)
        new_score = jnp.sum(wide.astype(F32) * new_key, axis=1, keepdims=True) * scale
        visible = position < len_ref[r]
        masked = jnp.where(visible, scores, -1e30)
        top = jnp.maximum(jnp.max(masked, axis=1, keepdims=True), new_score)
        exponent = jnp.where(visible, jnp.exp(masked - top), 0.0)
        new_exponent = jnp.exp(new_score - top)
        total = jnp.sum(exponent, axis=1, keepdims=True) + new_exponent
        mixed = jnp.dot(exponent.astype(BF16), kv_ref[1, r], preferred_element_type=F32)
        mixed = mixed + new_exponent.astype(BF16).astype(F32) * new_value
        mixed = jnp.where(own, mixed, 0.0)
        picked = mixed[:, :HD]
        for g in range(1, heads_kv):
            picked = picked + mixed[:, g * HD : (g + 1) * HD]
        scratch[pl.ds(r, heads, stride=dec_dev), :] = picked / total
    chunk = scratch.shape[0] // len(out_refs)
    for d, out in enumerate(out_refs):
        out[...] = scratch[pl.ds(pl.multiple_of((me ^ d) * chunk, 4), chunk), :].astype(BF16)


def attend_kernel(len_ref, *refs, ten, rows, prefix_rows, span_dev, heads_own, kv_own):
    packed, decoded, w_ref = refs[:ten], refs[ten : 2 * ten], refs[2 * ten]
    keep_ref, send_ref, att, w_vmem, sem = refs[2 * ten + 1 :]
    copy = pltpu.make_async_copy(w_ref, w_vmem, sem)
    copy.start()
    me = lax.axis_index("ten")
    dec_dev = rows - span_dev
    pieces = heads_own // kv_own
    scale = HD ** (-0.5)
    order = bit_reversed(ten)
    keys = ten * (prefix_rows + rows)
    prefix_keys = ten * prefix_rows
    row = lax.broadcasted_iota(jnp.int32, (ten * rows, 1), 0)
    col = lax.broadcasted_iota(jnp.int32, (1, keys), 1)
    row_pos = jnp.zeros((ten * rows, 1), jnp.int32)
    prefix_pos = jnp.full((1, keys), 1 << 30, jnp.int32)
    fresh_pos = jnp.full((1, keys), 1 << 30, jnp.int32)
    for b, d in enumerate(order):
        t = me ^ d
        i = row - b * rows
        row_pos = jnp.where((i >= 0) & (i < rows), t * span_dev + i, row_pos)
        p = col - b * prefix_rows
        prefix_pos = jnp.where((p >= 0) & (p < prefix_rows), t * prefix_rows + p, prefix_pos)
        f = col - prefix_keys - b * rows
        fresh_pos = jnp.where((f >= 0) & (f < span_dev), t * span_dev + f, fresh_pos)
    visible = (prefix_pos < len_ref[0]) | (fresh_pos <= row_pos)
    new_base = pieces * rows
    prefix_base = new_base + 2 * rows
    for g in range(kv_own):
        lanes = slice(g * HD, (g + 1) * HD)

        def gather(s):
            start = prefix_base + s * prefix_rows
            fresh = new_base + s * rows
            return jnp.concatenate(
                [packed[d][start : start + prefix_rows, lanes] for d in order]
                + [packed[d][fresh : fresh + rows, lanes] for d in order],
                axis=0,
            )

        key_rows, value_rows = gather(0), gather(1)
        for h in range(g * pieces, (g + 1) * pieces):
            piece, part = h // kv_own, h % kv_own
            q = jnp.concatenate(
                [
                    packed[d][piece * rows : (piece + 1) * rows, part * HD : (part + 1) * HD]
                    for d in order
                ],
                axis=0,
            )
            scores = (
                lax.dot_general(
                    q, key_rows, (((1,), (1,)), ((), ())), preferred_element_type=F32
                )
                * scale
            )
            masked = jnp.where(visible, scores, -1e30)
            top = jnp.max(masked, axis=1, keepdims=True)
            exponent = jnp.where(visible, jnp.exp(masked - top), 0.0)
            total = jnp.sum(exponent, axis=1, keepdims=True)
            out = jnp.dot(exponent.astype(BF16), value_rows, preferred_element_type=F32) / total
            att[:, h * HD : (h + 1) * HD] = out
            for b, d in enumerate(order):
                att[b * rows + span_dev : (b + 1) * rows, h * HD : (h + 1) * HD] = decoded[d][
                    h * dec_dev : (h + 1) * dec_dev, :
                ].astype(F32)
    half = ten * rows // 2
    copy.wait()
    attended = att[...].astype(BF16)
    step = 512
    for n in range(0, w_ref.shape[1], step):
        part = jnp.dot(attended, w_vmem[:, n : n + step], preferred_element_type=F32)
        keep_ref[:, n : n + step] = part[:half]
        send_ref[:, n : n + step] = part[half:].astype(BF16)


def route_kernel(*refs, parts, groups, local):
    addends = refs[:parts]
    hidden_ref, gain_ref, router_ref, ids_ref = refs[parts : parts + 4]
    residual_ref, map_ref = refs[parts + 4 : parts + 6]
    slot_refs = refs[parts + 6 :]
    me = lax.axis_index("exp")
    residual = hidden_ref[...].astype(F32)
    for a in addends:
        residual = residual + a[...].astype(F32)
    residual_ref[...] = residual
    rows, width = residual.shape
    mean_square = jnp.sum(residual * residual, axis=1, keepdims=True) / width
    normed = (residual * lax.rsqrt(mean_square + 1e-05) * gain_ref[...]).astype(BF16)
    logits = lax.dot_general(
        normed, router_ref[...], (((1,), (1,)), ((), ())), preferred_element_type=F32
    )
    first, second = ids_ref[:, 0:1], ids_ref[:, 1:2]
    expert = lax.broadcasted_iota(jnp.int32, logits.shape, 1)
    first_logit = jnp.sum(jnp.where(expert == first, logits, 0.0), axis=1, keepdims=True)
    second_logit = jnp.sum(jnp.where(expert == second, logits, 0.0), axis=1, keepdims=True)
    top = jnp.maximum(first_logit, second_logit)
    first_exp, second_exp = jnp.exp(first_logit - top), jnp.exp(second_logit - top)
    total = first_exp + second_exp
    slots = local * groups * SLOTS
    lane = lax.broadcasted_iota(jnp.int32, (rows, slots), 1)
    within = lane % SLOTS
    group = (lane // SLOTS) % groups
    slot_expert = (group ^ me) * local + lane // (SLOTS * groups)
    is_first, is_second = slot_expert == first, slot_expert == second
    named = is_first | is_second
    below = (
        lax.broadcasted_iota(jnp.int32, (rows, rows), 1)
        < lax.broadcasted_iota(jnp.int32, (rows, rows), 0)
    )
    rank = jnp.dot(
        jnp.where(below, 1.0, 0.0).astype(BF16),
        jnp.where(named, 1.0, 0.0).astype(BF16),
        preferred_element_type=F32,
    )
    placed = named & (rank == within.astype(F32))
    map_ref[...] = jnp.where(
        placed, jnp.where(is_first, first_exp / total, second_exp / total), 0.0
    )
    chosen = lax.dot_general(
        jnp.where(placed, 1.0, 0.0).astype(BF16),
        normed,
        (((0,), (0,)), ((), ())),
        preferred_element_type=F32,
    ).astype(BF16)
    for s, out in enumerate(slot_refs):
        out[...] = chosen[s * SLOTS : (s + 1) * SLOTS, :]


def expert_kernel(low_ref, high_ref, gate_ref, up_ref, down_ref, keep_ref, send_ref, acc, x_all):
    step = pl.program_id(0)
    half = low_ref.shape[0]

    @pl.when(step == 0)
    def _():
        x_all[:half, :] = low_ref[...]
        x_all[half:, :] = high_ref[...]

    x = x_all[...]
    gate = jnp.dot(x, gate_ref[0], preferred_element_type=F32)
    up = jnp.dot(x, up_ref[0], preferred_element_type=F32)
    hidden = (gate / (1.0 + jnp.exp(-gate)) * up).astype(BF16)
    part = jnp.dot(hidden, down_ref[0], preferred_element_type=F32)

    @pl.when(step == 0)
    def _():
        acc[...] = part

    @pl.when(step > 0)
    def _():
        acc[...] += part

    @pl.when(step == pl.num_programs(0) - 1)
    def _():
        keep_ref[...] = acc[:half, :]
        send_ref[...] = acc[half:, :].astype(BF16)


def add_kernel(*refs, parts):
    addends, outs = refs[:parts], refs[parts:]
    total = addends[0][...].astype(F32)
    for a in addends[1:]:
        total = total + a[...].astype(F32)
    rows = outs[0].shape[0]
    for i, out in enumerate(outs):
        out[...] = total[i * rows : (i + 1) * rows, :].astype(out.dtype)


def mix_kernel(residual_ref, map_ref, *refs):
    returned, out = refs[:-1], refs[-1]
    rows = residual_ref.shape[0]
    table = jnp.concatenate([r[...] for r in returned], axis=0)
    weights = map_ref[...]
    high = weights.astype(BF16)
    rest = weights - high.astype(F32)
    middle = rest.astype(BF16)
    low = (rest - middle.astype(F32)).astype(BF16)
    stacked = jnp.concatenate([high, middle, low], axis=0)
    mixed = jnp.dot(stacked, table, preferred_element_type=F32)
    total = mixed[:rows] + mixed[rows : 2 * rows] + mixed[2 * rows :]
    out[...] = (residual_ref[...] + total).astype(out.dtype)


def row_block(array, rows, index):
    return pl.BlockSpec((rows, array.shape[1]), lambda i: (index, 0))


def halves_down(keep, send, axis, size):
    addends = [keep]
    rows = keep.shape[0]
    for bit in up_bits(size):
        got = lax.ppermute(send, axis, xor_pairs(size, bit))
        addends.append(got)
        if bit * 2 < size:
            rows //= 2
            send = pl.pallas_call(
                functools.partial(add_kernel, parts=len(addends)),
                grid=(1,),
                in_specs=[row_block(a, rows, 1) for a in addends],
                out_specs=[row_block(keep, rows, 0)],
                out_shape=[jax.ShapeDtypeStruct((rows, keep.shape[1]), BF16)],
            )(*addends)[0]
    return addends, rows


def on_device(
    hidden_in,
    queries,
    new_kv,
    prefix_kv,
    decode_kv,
    prefix_len,
    decode_len,
    out_proj,
    norm_gain,
    router_w,
    expert_ids,
    w_gate,
    w_up,
    w_down,
):
    ten = lax.axis_size("ten")
    groups = lax.axis_size("exp")
    rows, width = hidden_in.shape
    dec_dev = decode_len.shape[0]
    span_dev = rows - dec_dev
    heads_q = queries.shape[1] // HD
    heads_kv = new_kv.shape[2] // HD
    per_kv = heads_q // heads_kv
    heads_own = heads_q // ten
    kv_own = max(1, heads_own // per_kv)
    prefix_rows = prefix_kv.shape[2]
    experts = router_w.shape[1]
    local = experts // groups
    shape = jax.ShapeDtypeStruct

    packed_rows = (heads_own // kv_own) * rows + 2 * rows + 2 * prefix_rows
    packed = pl.pallas_call(
        functools.partial(pack_kernel, heads_own=heads_own, per_kv=per_kv, kv_own=kv_own),
        in_specs=[VMEM] * 3,
        out_specs=[VMEM] * ten,
        out_shape=[shape((packed_rows, kv_own * HD), BF16)] * ten,
    )(queries, new_kv, prefix_kv)
    packed = [packed[0]] + [
        lax.ppermute(packed[d], "ten", xor_pairs(ten, d)) for d in range(1, ten)
    ]

    decoded = pl.pallas_call(
        functools.partial(decode_kernel, per_kv=per_kv, span_dev=span_dev),
        in_specs=[SMEM] + [VMEM] * 3,
        out_specs=[VMEM] * ten,
        out_shape=[shape((heads_own * dec_dev, HD), BF16)] * ten,
        scratch_shapes=[pltpu.VMEM((heads_q * dec_dev, HD), F32)],
    )(decode_len, queries[span_dev:].reshape(dec_dev * heads_q, HD), decode_kv, new_kv)
    decoded = [decoded[0]] + [
        lax.ppermute(decoded[d], "ten", xor_pairs(ten, d)) for d in range(1, ten)
    ]

    half = ten * rows // 2
    keep, send = pl.pallas_call(
        functools.partial(
            attend_kernel,
            ten=ten,
            rows=rows,
            prefix_rows=prefix_rows,
            span_dev=span_dev,
            heads_own=heads_own,
            kv_own=kv_own,
        ),
        in_specs=[SMEM] + [VMEM] * (2 * ten) + [ANY],
        out_specs=[VMEM, VMEM],
        out_shape=[shape((half, width), F32), shape((half, width), BF16)],
        scratch_shapes=[
            pltpu.VMEM((ten * rows, heads_own * HD), F32),
            pltpu.VMEM(out_proj.shape, BF16),
            pltpu.SemaphoreType.DMA,
        ],
    )(prefix_len, *packed, *decoded, out_proj)
    addends, _ = halves_down(keep, send, "ten", ten)

    slot_count = local * groups
    routed = pl.pallas_call(
        functools.partial(route_kernel, parts=len(addends), groups=groups, local=local),
        grid=(1,),
        in_specs=[row_block(a, rows, 0) for a in addends]
        + [
            row_block(hidden_in, rows, 0),
            pl.BlockSpec((1, width), lambda i: (0, 0)),
            pl.BlockSpec((experts, width), lambda i: (0, 0)),
            pl.BlockSpec((rows, 2), lambda i: (0, 0)),
        ],
        out_specs=[
            pl.BlockSpec((rows, width), lambda i: (0, 0)),
            pl.BlockSpec((rows, slot_count * SLOTS), lambda i: (0, 0)),
        ]
        + [pl.BlockSpec((SLOTS, width), lambda i: (0, 0))] * slot_count,
        out_shape=[shape((rows, width), F32), shape((rows, slot_count * SLOTS), F32)]
        + [shape((SLOTS, width), BF16)] * slot_count,
    )(*addends, hidden_in, norm_gain.reshape(1, width), router_w.T, expert_ids)
    residual, weight_map, slots = routed[0], routed[1], routed[2:]

    arrived = []
    for e in range(local):
        mine = slots[e * groups : (e + 1) * groups]
        arrived.append(
            [mine[0]]
            + [lax.ppermute(mine[d], "exp", xor_pairs(groups, d)) for d in range(1, groups)]
        )
    tile = min(256, w_gate.shape[2])
    steps = w_gate.shape[2] // tile
    returned = []
    for e in range(local):
        block = jnp.concatenate(arrived[e], axis=0)
        for bit in reversed(up_bits(ten)[1:]):
            block = jnp.concatenate([block, lax.ppermute(block, "ten", xor_pairs(ten, bit))], axis=0)
        other = lax.ppermute(block, "ten", xor_pairs(ten, 1))
        half = block.shape[0]
        keep, send = pl.pallas_call(
            expert_kernel,
            grid=(steps,),
            in_specs=[
                pl.BlockSpec((half, width), lambda i: (0, 0)),
                pl.BlockSpec((half, width), lambda i: (0, 0)),
                pl.BlockSpec((1, width, tile), functools.partial(lambda e, i: (e, 0, i), e)),
                pl.BlockSpec((1, width, tile), functools.partial(lambda e, i: (e, 0, i), e)),
                pl.BlockSpec((1, tile, width), functools.partial(lambda e, i: (e, i, 0), e)),
            ],
            out_specs=[pl.BlockSpec((half, width), lambda i: (0, 0))] * 2,
            out_shape=[shape((half, width), F32), shape((half, width), BF16)],
            scratch_shapes=[
                pltpu.VMEM((2 * half, width), F32),
                pltpu.VMEM((2 * half, width), BF16),
            ],
        )(block, other, w_gate, w_up, w_down)
        addends, share = halves_down(keep, send, "ten", ten)
        pieces = pl.pallas_call(
            functools.partial(add_kernel, parts=len(addends)),
            grid=(1,),
            in_specs=[row_block(a, share, 0) for a in addends],
            out_specs=[pl.BlockSpec((SLOTS, width), lambda i: (0, 0))] * groups,
            out_shape=[shape((SLOTS, width), BF16)] * groups,
        )(*addends)
        returned.append(pieces[0])
        returned += [
            lax.ppermute(pieces[d], "exp", xor_pairs(groups, d)) for d in range(1, groups)
        ]
    return pl.pallas_call(
        mix_kernel,
        in_specs=[VMEM] * (2 + len(returned)),
        out_specs=VMEM,
        out_shape=shape((rows, width), BF16),
    )(residual, weight_map, *returned)


def solution(mesh):
    in_specs = (
        P(("rep", "exp", "ten"), None),
        P(("rep", "exp", "ten"), None),
        P(None, ("rep", "exp", "ten"), None),
        P(None, ("rep", "exp"), "ten", None),
        P(None, ("rep", "exp", "ten"), None, None),
        P(("rep", "exp")),
        P(("rep", "exp", "ten")),
        P("ten", None),
        P(),
        P(),
        P(("rep", "exp", "ten"), None),
        P("exp", None, "ten"),
        P("exp", None, "ten"),
        P("exp", "ten", None),
    )
    out_specs = P(("rep", "exp", "ten"), None)
    return jax.shard_map(
        on_device, mesh=mesh, in_specs=in_specs, out_specs=out_specs, check_vma=False
    )
```

```python
import functools

import jax
import jax.numpy as jnp
from jax import lax
from jax.experimental import pallas as pl
from jax.experimental.pallas import tpu as pltpu
from jax.sharding import PartitionSpec as P

HD = 128
SLOTS = 8
F32 = jnp.float32
BF16 = jnp.bfloat16
MIB = 2**20
VMEM = pl.BlockSpec(memory_space=pltpu.VMEM)
SMEM = pl.BlockSpec(memory_space=pltpu.SMEM)
HBM = pl.BlockSpec(memory_space=pltpu.HBM)


def xor_pairs(size, distance):
    return [(i, i ^ distance) for i in range(size)]


def bit_reversed(size):
    order = [0]
    step = size // 2
    while step:
        order = order + [o + step for o in order]
        step //= 2
    return order


def up_bits(size):
    return [1 << b for b in range(size.bit_length() - 1)]


def out(shape, dtype):
    return jax.ShapeDtypeStruct(shape, dtype)


def held(array):
    return pltpu.with_memory_space_constraint(array, pltpu.VMEM)


def call(kernel, args, specs, outs, scratch=(), limit=4, flops=0, aliases=None):
    limit *= max(1, lax.axis_size("ten") * lax.axis_size("exp") // 16)
    args = [
        pltpu.with_memory_space_constraint(a, pltpu.HBM) if s is HBM else a
        for a, s in zip(args, specs)
    ]
    return pl.pallas_call(
        kernel,
        in_specs=specs,
        out_specs=[VMEM] * len(outs),
        out_shape=outs,
        scratch_shapes=list(scratch),
        compiler_params=pltpu.CompilerParams(vmem_limit_bytes=limit * MIB),
        cost_estimate=pl.CostEstimate(flops=flops, bytes_accessed=0, transcendentals=0),
        input_output_aliases=aliases or {},
    )(*args)


def load_all(pairs, sems):
    copies = [pltpu.make_async_copy(a, b, sems.at[i]) for i, (a, b) in enumerate(pairs)]
    for copy in copies:
        copy.start()
    return copies


def pack_kernel(q_hbm, new_hbm, prefix_hbm, *refs, heads_own, per_kv, kv_own):
    out_refs, (q_ref, new_ref, prefix_ref, sems) = refs[:-4], refs[-4:]
    pairs = ((q_hbm, q_ref), (new_hbm, new_ref), (prefix_hbm, prefix_ref))
    for copy in load_all(pairs, sems):
        copy.wait()
    me = lax.axis_index("ten")
    rows = q_ref.shape[0]
    prefix_rows = prefix_ref.shape[2]
    width = kv_own * HD
    pieces = heads_own // kv_own
    for d, out in enumerate(out_refs):
        t = me ^ d
        q_start = pl.multiple_of(t * (heads_own * HD), HD)
        for j in range(pieces):
            out[j * rows : (j + 1) * rows, :] = q_ref[
                :, pl.ds(pl.multiple_of(q_start + j * width, HD), width)
            ]
        kv_start = pl.multiple_of(((t * heads_own) // per_kv) * HD, HD)
        base = pieces * rows
        for s in range(2):
            out[base : base + rows, :] = new_ref[s, :, pl.ds(kv_start, width)]
            base += rows
        for s in range(2):
            out[base : base + prefix_rows, :] = prefix_ref[s, 0, :, pl.ds(kv_start, width)]
            base += prefix_rows


def decode_kernel(len_ref, q_ref, kv_hbm, new_hbm, *refs, per_kv, span_dev):
    out_refs, (kv_ref, new_ref, scratch, sems) = refs[:-4], refs[-4:]
    for copy in load_all(((kv_hbm, kv_ref), (new_hbm, new_ref)), sems):
        copy.wait()
    me = lax.axis_index("ten")
    dec_dev, ctx_len, kv_width = kv_ref.shape[1:]
    heads = q_ref.shape[0] // dec_dev
    heads_kv = kv_width // HD
    scale = HD ** (-0.5)
    row_group = lax.broadcasted_iota(jnp.int32, (heads, kv_width), 0) // per_kv
    lane_group = lax.broadcasted_iota(jnp.int32, (heads, kv_width), 1) // HD
    own = row_group == lane_group
    position = lax.broadcasted_iota(jnp.int32, (heads, ctx_len), 1)
    for r in range(dec_dev):
        q = q_ref[r * heads : (r + 1) * heads, :]
        wide = jnp.where(own, jnp.concatenate([q] * heads_kv, axis=1), jnp.zeros((), BF16))
        scores = (
            lax.dot_general(
                wide, kv_ref[0, r], (((1,), (1,)), ((), ())), preferred_element_type=F32
            )
            * scale
        )
        new_key = new_ref[0, span_dev + r : span_dev + r + 1, :].astype(F32)
        new_value = new_ref[1, span_dev + r : span_dev + r + 1, :].astype(F32)
        new_score = jnp.sum(wide.astype(F32) * new_key, axis=1, keepdims=True) * scale
        visible = position < len_ref[r]
        masked = jnp.where(visible, scores, -1e30)
        top = jnp.maximum(jnp.max(masked, axis=1, keepdims=True), new_score)
        exponent = jnp.where(visible, jnp.exp(masked - top), 0.0)
        new_exponent = jnp.exp(new_score - top)
        total = jnp.sum(exponent, axis=1, keepdims=True) + new_exponent
        mixed = jnp.dot(exponent.astype(BF16), kv_ref[1, r], preferred_element_type=F32)
        mixed = mixed + new_exponent.astype(BF16).astype(F32) * new_value
        mixed = jnp.where(own, mixed, 0.0)
        picked = mixed[:, :HD]
        for g in range(1, heads_kv):
            picked = picked + mixed[:, g * HD : (g + 1) * HD]
        scratch[pl.ds(r, heads, stride=dec_dev), :] = picked / total
    chunk = scratch.shape[0] // len(out_refs)
    for d, out in enumerate(out_refs):
        out[...] = scratch[pl.ds(pl.multiple_of((me ^ d) * chunk, 4), chunk), :].astype(BF16)


def attend_kernel(len_ref, *refs, ten, rows, prefix_rows, span_dev, heads_own, kv_own):
    packed, decoded = refs[:ten], refs[ten : 2 * ten]
    w_ref, ahead_ref, _ = refs[2 * ten : 2 * ten + 3]
    keep_ref, send_ref, ahead_out, att, sem = refs[2 * ten + 3 :]
    copy = pltpu.make_async_copy(ahead_ref.at[0], ahead_out, sem)
    copy.start()
    me = lax.axis_index("ten")
    dec_dev = rows - span_dev
    pieces = heads_own // kv_own
    scale = HD ** (-0.5)
    order = bit_reversed(ten)
    keys = ten * (prefix_rows + rows)
    prefix_keys = ten * prefix_rows
    all_rows = ten * rows
    row = lax.broadcasted_iota(jnp.int32, (all_rows, 1), 0)
    col = lax.broadcasted_iota(jnp.int32, (1, keys), 1)
    row_pos = jnp.zeros((all_rows, 1), jnp.int32)
    prefix_pos = jnp.full((1, keys), 1 << 30, jnp.int32)
    fresh_pos = jnp.full((1, keys), 1 << 30, jnp.int32)
    for b, d in enumerate(order):
        t = me ^ d
        i = row - b * rows
        row_pos = jnp.where((i >= 0) & (i < rows), t * span_dev + i, row_pos)
        p = col - b * prefix_rows
        prefix_pos = jnp.where((p >= 0) & (p < prefix_rows), t * prefix_rows + p, prefix_pos)
        f = col - prefix_keys - b * rows
        fresh_pos = jnp.where((f >= 0) & (f < span_dev), t * span_dev + f, fresh_pos)
    visible = (prefix_pos < len_ref[0]) | (fresh_pos <= row_pos)
    bias = jnp.where(visible, 0.0, -1e30)
    bias = jnp.concatenate([bias] * pieces, axis=0)
    new_base = pieces * rows
    prefix_base = new_base + 2 * rows
    for g in range(kv_own):
        lanes = slice(g * HD, (g + 1) * HD)

        def gather(s):
            start = prefix_base + s * prefix_rows
            fresh = new_base + s * rows
            return jnp.concatenate(
                [packed[d][start : start + prefix_rows, lanes] for d in order]
                + [packed[d][fresh : fresh + rows, lanes] for d in order],
                axis=0,
            )

        heads = range(g * pieces, (g + 1) * pieces)
        q = jnp.concatenate(
            [
                packed[d][
                    (h // kv_own) * rows : (h // kv_own + 1) * rows,
                    (h % kv_own) * HD : (h % kv_own + 1) * HD,
                ]
                for h in heads
                for d in order
            ],
            axis=0,
        )
        scores = (
            lax.dot_general(q, gather(0), (((1,), (1,)), ((), ())), preferred_element_type=F32)
            * scale
            + bias
        )
        top = jnp.max(scores, axis=1, keepdims=True)
        exponent = jnp.exp(scores - top)
        total = jnp.sum(exponent, axis=1, keepdims=True)
        out = jnp.dot(exponent.astype(BF16), gather(1), preferred_element_type=F32) / total
        for n, h in enumerate(heads):
            att[:, h * HD : (h + 1) * HD] = out[n * all_rows : (n + 1) * all_rows]
            for b, d in enumerate(order):
                att[b * rows + span_dev : (b + 1) * rows, h * HD : (h + 1) * HD] = decoded[d][
                    h * dec_dev : (h + 1) * dec_dev, :
                ].astype(F32)
    half = all_rows // 2
    attended = att[...].astype(BF16)
    step = 512
    for n in range(0, w_ref.shape[1], step):
        part = jnp.dot(attended, w_ref[:, n : n + step], preferred_element_type=F32)
        keep_ref[:, n : n + step] = part[:half]
        send_ref[:, n : n + step] = part[half:].astype(BF16)
    copy.wait()


def route_kernel(*refs, parts, groups, local, rows):
    addends = refs[:parts]
    hidden_ref, gain_ref, router_ref, ids_ref, _ = refs[parts : parts + 5]
    residual_ref, map_ref = refs[parts + 5 : parts + 7]
    slot_refs = refs[parts + 7 :]
    me = lax.axis_index("exp")
    residual = hidden_ref[...].astype(F32)
    for a in addends:
        residual = residual + a[:rows, :].astype(F32)
    residual_ref[...] = residual
    width = residual.shape[1]
    mean_square = jnp.sum(residual * residual, axis=1, keepdims=True) / width
    normed = (residual * lax.rsqrt(mean_square + 1e-05) * gain_ref[...]).astype(BF16)
    logits = lax.dot_general(
        normed, router_ref[...], (((1,), (1,)), ((), ())), preferred_element_type=F32
    )
    diagonal = lax.broadcasted_iota(jnp.int32, (rows, rows), 0) == lax.broadcasted_iota(
        jnp.int32, (rows, rows), 1
    )
    first, second = (
        jnp.sum(jnp.where(diagonal, ids_ref[k : k + 1, :], 0), axis=1, keepdims=True)
        for k in range(2)
    )
    expert = lax.broadcasted_iota(jnp.int32, logits.shape, 1)
    first_logit = jnp.sum(jnp.where(expert == first, logits, 0.0), axis=1, keepdims=True)
    second_logit = jnp.sum(jnp.where(expert == second, logits, 0.0), axis=1, keepdims=True)
    top = jnp.maximum(first_logit, second_logit)
    first_exp, second_exp = jnp.exp(first_logit - top), jnp.exp(second_logit - top)
    total = first_exp + second_exp
    slots = local * groups * SLOTS
    lane = lax.broadcasted_iota(jnp.int32, (rows, slots), 1)
    within = lane % SLOTS
    group = lane // (SLOTS * local)
    slot_expert = (group ^ me) * local + (lane // SLOTS) % local
    is_first, is_second = slot_expert == first, slot_expert == second
    named = is_first | is_second
    below = (
        lax.broadcasted_iota(jnp.int32, (rows, rows), 1)
        < lax.broadcasted_iota(jnp.int32, (rows, rows), 0)
    )
    rank = jnp.dot(
        jnp.where(below, 1.0, 0.0).astype(BF16),
        jnp.where(named, 1.0, 0.0).astype(BF16),
        preferred_element_type=F32,
    )
    placed = named & (rank == within.astype(F32))
    map_ref[...] = jnp.where(
        placed, jnp.where(is_first, first_exp / total, second_exp / total), 0.0
    )
    chosen = lax.dot_general(
        jnp.where(placed, 1.0, 0.0).astype(BF16),
        normed,
        (((0,), (0,)), ((), ())),
        preferred_element_type=F32,
    ).astype(BF16)
    block = local * SLOTS
    for s, out in enumerate(slot_refs):
        out[...] = chosen[s * block : (s + 1) * block, :]


def hidden_kernel(*refs, pieces, expert, tile, resident, last):
    xs, refs = refs[:pieces], refs[pieces:]
    if resident:
        gate_ref, up_ref, refs = refs[0], refs[1], refs[2:]
    else:
        gate_low, gate_high, up_low, up_hbm, down_hbm = refs[:5]
        refs = refs[5:]
    if not last:
        next_gate, refs = refs[0], refs[1:]
    hidden_ref, refs = refs[0], refs[1:]
    if not resident:
        up_rest, down_low, refs = refs[0], refs[1], refs[2:]
    if not last:
        next_low, refs = refs[0], refs[1:]
    x_all, sems = refs
    pending = []

    def start(source, target, n):
        pending.append(pltpu.make_async_copy(source, target, sems.at[n]))
        pending[-1].start()

    tiles = hidden_ref.shape[1] // tile
    up_copies = []
    if not resident:
        for i in range(1, tiles):
            up_copies.append(
                pltpu.make_async_copy(
                    up_hbm.at[expert, :, pl.ds(i * tile, tile)],
                    up_rest.at[:, pl.ds((i - 1) * tile, tile)],
                    sems.at[i],
                )
            )
            up_copies[-1].start()
    if not last:
        start(next_gate.at[expert + 1, :, pl.ds(0, next_low.shape[1])], next_low, 0)
    for i, p in enumerate(xs):
        x_all[i * SLOTS : (i + 1) * SLOTS, :] = p[expert * SLOTS : (expert + 1) * SLOTS, :]
    for i in range(tiles):
        cols = slice(i * tile, (i + 1) * tile)
        if resident:
            gate_tile = gate_ref[:, cols]
        else:
            gate_tile = gate_low[:, cols] if i < tiles - 1 else gate_high[...]
        gate = jnp.dot(x_all[...], gate_tile, preferred_element_type=F32)
        if resident:
            up_tile = up_ref[:, cols]
        elif i == 0:
            up_tile = up_low[...]
        else:
            up_copies[i - 1].wait()
            if i == tiles - 1:
                start(down_hbm.at[expert, :, pl.ds(0, down_low.shape[1])], down_low, tiles)
            up_tile = up_rest[:, (i - 1) * tile : i * tile]
        up = jnp.dot(x_all[...], up_tile, preferred_element_type=F32)
        hidden_ref[:, cols] = (gate / (1.0 + jnp.exp(-gate)) * up).astype(BF16)
    for copy in pending:
        copy.wait()


def down_kernel(hidden_ref, down_ref, *refs, resident, last, expert, tile, extra):
    if not resident:
        down_hbm, refs = refs[0], refs[1 + extra :]
    if not last:
        next_gate, next_up, refs = refs[0], refs[1], refs[2:]
    keep_ref, send_ref, refs = refs[0], refs[1], refs[2:]
    if not resident:
        rest_ref, refs = refs[0], refs[1:]
    if not last:
        gate_high, up_low, refs = refs[0], refs[1], refs[2:]
    sems = refs[0]
    split = down_ref.shape[1]
    half, width = keep_ref.shape
    pending = []
    if not last:
        low = next_gate.shape[2] - tile
        pending = load_all(
            (
                (next_gate.at[expert + 1, :, pl.ds(low, tile)], gate_high),
                (next_up.at[expert + 1, :, pl.ds(0, tile)], up_low),
            ),
            sems,
        )
    copies = []
    if not resident:
        for i in range((width - split) // tile):
            copies.append(
                pltpu.make_async_copy(
                    down_hbm.at[expert, :, pl.ds(split + i * tile, tile)],
                    rest_ref.at[:, pl.ds(i * tile, tile)],
                    sems.at[2 + i],
                )
            )
            copies[-1].start()
    for start in range(0, width, tile):
        cols = slice(start, start + tile)
        if start >= split:
            i = (start - split) // tile
            copies[i].wait()
            down_tile = rest_ref[:, i * tile : (i + 1) * tile]
        else:
            down_tile = down_ref[:, cols]
        part = jnp.dot(hidden_ref[...], down_tile, preferred_element_type=F32)
        keep_ref[:, cols] = part[:half]
        send_ref[:, cols] = part[half:].astype(BF16)
    for copy in pending:
        copy.wait()


def add_kernel(*refs, parts, first, rows, skip=0):
    addends, outs = refs[:parts], refs[parts + skip :]
    total = addends[0][first : first + rows, :].astype(F32)
    for a in addends[1:]:
        total = total + a[first : first + rows, :].astype(F32)
    each = outs[0].shape[0]
    for i, out in enumerate(outs):
        out[...] = total[i * each : (i + 1) * each, :].astype(out.dtype)


def mix_kernel(residual_ref, map_ref, *refs, local, groups):
    returned, out = refs[:-1], refs[-1]
    rows = residual_ref.shape[0]
    table = jnp.concatenate(
        [returned[e * groups + d][...] for d in range(groups) for e in range(local)], axis=0
    )
    weights = map_ref[...]
    high = weights.astype(BF16)
    rest = weights - high.astype(F32)
    middle = rest.astype(BF16)
    low = (rest - middle.astype(F32)).astype(BF16)
    stacked = jnp.concatenate([high, middle, low], axis=0)
    mixed = jnp.dot(stacked, table, preferred_element_type=F32)
    total = mixed[:rows] + mixed[rows : 2 * rows] + mixed[2 * rows :]
    out[...] = (residual_ref[...] + total).astype(out.dtype)


def fetch_kernel(source_ref, _, out_ref, token_ref, sem, *, expert):
    source = source_ref if expert is None else source_ref.at[expert]
    copy = pltpu.make_async_copy(source.at[:, pl.ds(0, out_ref.shape[1])], out_ref, sem)
    copy.start()
    token_ref[...] = jnp.zeros_like(token_ref)
    copy.wait()


def fetch(source, expert, after, columns=None):
    rows, width = source.shape[-2:]
    return call(
        functools.partial(fetch_kernel, expert=expert),
        (source, after),
        [HBM, VMEM],
        [out((rows, columns or width), BF16), out((8, HD), F32)],
        [pltpu.SemaphoreType.DMA],
        limit=2,
    )


def send_to(x, axis, distance):
    return lax.ppermute(x, axis, xor_pairs(lax.axis_size(axis), distance))


def halves_down(keep, send, axis, size):
    addends = [keep]
    rows = keep.shape[0]
    last_sent = send
    for bit in up_bits(size):
        addends.append(send_to(send, axis, bit))
        last_sent = send
        if bit * 2 < size:
            rows //= 2
            send = call(
                functools.partial(add_kernel, parts=len(addends), first=rows, rows=rows),
                addends,
                [VMEM] * len(addends),
                [out((rows, keep.shape[1]), BF16)],
                limit=3,
            )[0]
    return addends, rows, last_sent


def on_device(
    hidden_in,
    queries,
    new_kv,
    prefix_kv,
    decode_kv,
    prefix_len,
    decode_len,
    out_proj,
    norm_gain,
    router_w,
    expert_ids,
    w_gate,
    w_up,
    w_down,
):
    ten = lax.axis_size("ten")
    groups = lax.axis_size("exp")
    rows, width = hidden_in.shape
    dec_dev = decode_len.shape[0]
    span_dev = rows - dec_dev
    heads_q = queries.shape[1] // HD
    heads_kv = new_kv.shape[2] // HD
    per_kv = heads_q // heads_kv
    heads_own = heads_q // ten
    kv_own = max(1, heads_own // per_kv)
    prefix_rows = prefix_kv.shape[2]
    experts = router_w.shape[1]
    local = experts // groups

    packed_rows = (heads_own // kv_own) * rows + 2 * rows + 2 * prefix_rows
    packed = call(
        functools.partial(pack_kernel, heads_own=heads_own, per_kv=per_kv, kv_own=kv_own),
        (queries, new_kv, prefix_kv),
        [HBM] * 3,
        [out((packed_rows, kv_own * HD), BF16)] * ten,
        [pltpu.VMEM(a.shape, BF16) for a in (queries, new_kv, prefix_kv)]
        + [pltpu.SemaphoreType.DMA((3,))],
    )
    packed = [packed[0]] + [
        lax.ppermute(packed[d], "ten", xor_pairs(ten, d)) for d in range(1, ten)
    ]

    decoded = call(
        functools.partial(decode_kernel, per_kv=per_kv, span_dev=span_dev),
        (
            decode_len,
            queries[span_dev:].reshape(dec_dev * heads_q, HD),
            decode_kv,
            new_kv,
        ),
        [SMEM, VMEM, HBM, HBM],
        [out((heads_own * dec_dev, HD), BF16)] * ten,
        [
            pltpu.VMEM(decode_kv.shape, BF16),
            pltpu.VMEM(new_kv.shape, BF16),
            pltpu.VMEM((heads_q * dec_dev, HD), F32),
            pltpu.SemaphoreType.DMA((2,)),
        ],
        limit=4,
    )
    own_decoded = decoded[0]
    decoded = [decoded[0]] + [
        lax.ppermute(decoded[d], "ten", xor_pairs(ten, d)) for d in range(1, ten)
    ]
    proj, proj_token = fetch(out_proj, None, own_decoded)

    half = ten * rows // 2
    keep, send, up = call(
        functools.partial(
            attend_kernel,
            ten=ten,
            rows=rows,
            prefix_rows=prefix_rows,
            span_dev=span_dev,
            heads_own=heads_own,
            kv_own=kv_own,
        ),
        (prefix_len, *packed, *decoded, held(proj), w_up, proj_token),
        [SMEM] + [VMEM] * (2 * ten) + [VMEM, HBM, VMEM],
        [
            out((half, width), F32),
            out((half, width), BF16),
            out(w_up.shape[1:], BF16),
        ],
        [pltpu.VMEM((ten * rows, heads_own * HD), F32), pltpu.SemaphoreType.DMA],
        limit=4,
    )
    addends, _, last_sent = halves_down(keep, send, "ten", ten)
    down, down_token = fetch(w_down, 0, last_sent)

    routed = call(
        functools.partial(
            route_kernel, parts=len(addends), groups=groups, local=local, rows=rows
        ),
        (
            *addends,
            hidden_in,
            norm_gain.reshape(1, width),
            router_w.T,
            expert_ids.T,
            down_token,
        ),
        [VMEM] * (len(addends) + 5),
        [out((rows, width), F32), out((rows, experts * SLOTS), F32)]
        + [out((local * SLOTS, width), BF16)] * groups,
        limit=3,
    )
    residual, weight_map, slots = routed[0], routed[1], routed[2:]

    block = [slots[0]] + [send_to(slots[d], "exp", d) for d in range(1, groups)]
    for bit in reversed(up_bits(ten)):
        block = block + [send_to(b, "ten", bit) for b in block]

    gate, _ = fetch(w_gate, 0, slots[0])
    hidden_units = w_gate.shape[2]
    tile = min(512, hidden_units // 4)
    tiles = hidden_units // tile
    down_low_width = 2 * tile
    half = len(block) * SLOTS // 2
    returned = []
    for e in range(local):
        last, resident = e == local - 1, e == 0
        args, specs = [*block], [VMEM] * len(block)
        outs = [out((2 * half, hidden_units), BF16)]
        if resident:
            args += [held(gate), held(up)]
            specs += [VMEM] * 2
        else:
            args += [held(next_low), held(gate_high), held(up_low), w_up, w_down]
            specs += [VMEM] * 3 + [HBM] * 2
            outs += [
                out((width, hidden_units - tile), BF16),
                out((hidden_units, down_low_width), BF16),
            ]
        if not last:
            args.append(w_gate)
            specs.append(HBM)
            outs.append(out((width, hidden_units - tile), BF16))
        hidden, *rest = call(
            functools.partial(
                hidden_kernel,
                pieces=len(block),
                expert=e,
                tile=tile,
                resident=resident,
                last=last,
            ),
            args,
            specs,
            outs,
            [pltpu.VMEM((2 * half, width), BF16), pltpu.SemaphoreType.DMA((tiles + 1,))],
            limit=3,
            flops=8 * half * width * hidden_units,
        )
        if not last:
            next_low = rest[-1]
        args, specs = [hidden], [VMEM]
        outs = [out((half, width), F32), out((half, width), BF16)]
        if resident:
            args.append(held(down))
            specs.append(VMEM)
        else:
            args += [held(rest[1]), w_down, rest[0], before]
            specs += [VMEM, HBM, VMEM, VMEM]
            outs.append(out((hidden_units, width - down_low_width), BF16))
        if not last:
            args += [w_gate, w_up]
            specs += [HBM, HBM]
            outs += [out((width, tile), BF16)] * 2
        keep, send, *rest = call(
            functools.partial(
                down_kernel, resident=resident, last=last, expert=e, tile=tile, extra=2
            ),
            args,
            specs,
            outs,
            [pltpu.SemaphoreType.DMA((2 + width // tile,))],
            limit=3,
            flops=4 * half * width * hidden_units,
        )
        if not last:
            gate_high, up_low = rest[-2:]
            rest = rest[:-2]
        addends, share, before = halves_down(keep, send, "ten", ten)
        pieces = call(
            functools.partial(
                add_kernel, parts=len(addends), first=0, rows=share, skip=len(rest)
            ),
            (*addends, *rest),
            [VMEM] * (len(addends) + len(rest)),
            [out((SLOTS, width), BF16)] * groups,
            limit=3,
        )
        returned.append(pieces[0])
        returned += [
            lax.ppermute(pieces[d], "exp", xor_pairs(groups, d)) for d in range(1, groups)
        ]
    return pl.pallas_call(
        functools.partial(mix_kernel, local=local, groups=groups),
        in_specs=[VMEM] * (2 + len(returned)),
        out_specs=VMEM,
        out_shape=jax.ShapeDtypeStruct((rows, width), BF16),
        compiler_params=pltpu.CompilerParams(vmem_limit_bytes=16 * MIB),
        name="mix",
    )(residual, weight_map, *returned)


def solution(mesh):
    in_specs = (
        P(("rep", "exp", "ten"), None),
        P(("rep", "exp", "ten"), None),
        P(None, ("rep", "exp", "ten"), None),
        P(None, ("rep", "exp"), "ten", None),
        P(None, ("rep", "exp", "ten"), None, None),
        P(("rep", "exp")),
        P(("rep", "exp", "ten")),
        P("ten", None),
        P(),
        P(),
        P(("rep", "exp", "ten"), None),
        P("exp", None, "ten"),
        P("exp", None, "ten"),
        P("exp", "ten", None),
    )
    out_specs = P(("rep", "exp", "ten"), None)

    return jax.shard_map(
        on_device, mesh=mesh, in_specs=in_specs, out_specs=out_specs, check_vma=False
    )
```

```python
import functools

import jax
import jax.numpy as jnp
from jax import lax
from jax.experimental import pallas as pl
from jax.experimental.pallas import tpu as pltpu
from jax.sharding import PartitionSpec as P

HD = 128
SLOTS = 8
F32 = jnp.float32
BF16 = jnp.bfloat16
MIB = 2**20
VMEM = pl.BlockSpec(memory_space=pltpu.VMEM)
SMEM = pl.BlockSpec(memory_space=pltpu.SMEM)
HBM = pl.BlockSpec(memory_space=pltpu.HBM)


def xor_pairs(size, distance):
    return [(i, i ^ distance) for i in range(size)]


def bit_reversed(size):
    order = [0]
    step = size // 2
    while step:
        order = order + [o + step for o in order]
        step //= 2
    return order


def up_bits(size):
    return [1 << b for b in range(size.bit_length() - 1)]


def out(shape, dtype):
    return jax.ShapeDtypeStruct(shape, dtype)


def held(array):
    return pltpu.with_memory_space_constraint(array, pltpu.VMEM)


def call(kernel, args, specs, outs, scratch=(), limit=4, flops=0, aliases=None):
    limit *= max(1, lax.axis_size("ten") * lax.axis_size("exp") // 16)
    args = [
        pltpu.with_memory_space_constraint(a, pltpu.HBM) if s is HBM else a
        for a, s in zip(args, specs)
    ]
    return pl.pallas_call(
        kernel,
        in_specs=specs,
        out_specs=[VMEM] * len(outs),
        out_shape=outs,
        scratch_shapes=list(scratch),
        compiler_params=pltpu.CompilerParams(vmem_limit_bytes=limit * MIB),
        cost_estimate=pl.CostEstimate(flops=flops, bytes_accessed=0, transcendentals=0),
        input_output_aliases=aliases or {},
    )(*args)


def load_all(pairs, sems):
    copies = [pltpu.make_async_copy(a, b, sems.at[i]) for i, (a, b) in enumerate(pairs)]
    for copy in copies:
        copy.start()
    return copies


def pack_kernel(q_hbm, new_hbm, prefix_hbm, *refs, heads_own, per_kv, kv_own):
    out_refs, (q_ref, new_ref, prefix_ref, sems) = refs[:-4], refs[-4:]
    pairs = ((q_hbm, q_ref), (new_hbm, new_ref), (prefix_hbm, prefix_ref))
    for copy in load_all(pairs, sems):
        copy.wait()
    me = lax.axis_index("ten")
    rows = q_ref.shape[0]
    prefix_rows = prefix_ref.shape[2]
    width = kv_own * HD
    pieces = heads_own // kv_own
    for d, out in enumerate(out_refs):
        t = me ^ d
        q_start = pl.multiple_of(t * (heads_own * HD), HD)
        for j in range(pieces):
            out[j * rows : (j + 1) * rows, :] = q_ref[
                :, pl.ds(pl.multiple_of(q_start + j * width, HD), width)
            ]
        kv_start = pl.multiple_of(((t * heads_own) // per_kv) * HD, HD)
        base = pieces * rows
        for s in range(2):
            out[base : base + rows, :] = new_ref[s, :, pl.ds(kv_start, width)]
            base += rows
        for s in range(2):
            out[base : base + prefix_rows, :] = prefix_ref[s, 0, :, pl.ds(kv_start, width)]
            base += prefix_rows


def decode_kernel(len_hbm, q_hbm, kv_hbm, new_hbm, w_hbm, *refs, per_kv, span_dev, block):
    out_refs, (w_low, len_ref, q_ref, kv_ref, new_ref, q_heads, scratch, sems) = refs[:-8], refs[-8:]
    q_rows = q_hbm.at[pl.ds(q_hbm.shape[0] - block, block)]
    pairs = ((len_hbm, len_ref), (q_rows, q_ref), (kv_hbm, kv_ref), (new_hbm, new_ref))
    loads = load_all(pairs, sems)
    w_copy = pltpu.make_async_copy(
        w_hbm.at[:, pl.ds(0, w_low.shape[1])], w_low, sems.at[len(pairs)]
    )
    w_copy.start()
    for copy in loads:
        copy.wait()
    me = lax.axis_index("ten")
    dec_dev, ctx_len, kv_width = kv_ref.shape[1:]
    heads = q_ref.shape[1] // HD
    heads_kv = kv_width // HD
    for h in range(heads):
        q_heads[h * dec_dev : (h + 1) * dec_dev, :] = q_ref[
            block - dec_dev :, h * HD : (h + 1) * HD
        ].astype(F32)
    scale = HD ** (-0.5)
    row_group = lax.broadcasted_iota(jnp.int32, (heads, kv_width), 0) // per_kv
    lane_group = lax.broadcasted_iota(jnp.int32, (heads, kv_width), 1) // HD
    own = row_group == lane_group
    position = lax.broadcasted_iota(jnp.int32, (heads, ctx_len), 1)
    for r in range(dec_dev):
        q = q_heads[pl.ds(r, heads, stride=dec_dev), :].astype(BF16)
        wide = jnp.where(own, jnp.concatenate([q] * heads_kv, axis=1), jnp.zeros((), BF16))
        scores = (
            lax.dot_general(
                wide, kv_ref[0, r], (((1,), (1,)), ((), ())), preferred_element_type=F32
            )
            * scale
        )
        new_key = new_ref[0, span_dev + r : span_dev + r + 1, :].astype(F32)
        new_value = new_ref[1, span_dev + r : span_dev + r + 1, :].astype(F32)
        new_score = jnp.sum(wide.astype(F32) * new_key, axis=1, keepdims=True) * scale
        visible = position < len_ref[r]
        masked = jnp.where(visible, scores, -1e30)
        top = jnp.maximum(jnp.max(masked, axis=1, keepdims=True), new_score)
        exponent = jnp.where(visible, jnp.exp(masked - top), 0.0)
        new_exponent = jnp.exp(new_score - top)
        total = jnp.sum(exponent, axis=1, keepdims=True) + new_exponent
        mixed = jnp.dot(exponent.astype(BF16), kv_ref[1, r], preferred_element_type=F32)
        mixed = mixed + new_exponent.astype(BF16).astype(F32) * new_value
        mixed = jnp.where(own, mixed, 0.0)
        picked = mixed[:, :HD]
        for g in range(1, heads_kv):
            picked = picked + mixed[:, g * HD : (g + 1) * HD]
        scratch[pl.ds(r, heads, stride=dec_dev), :] = picked / total
    chunk = scratch.shape[0] // len(out_refs)
    for d, out in enumerate(out_refs):
        out[...] = scratch[pl.ds(pl.multiple_of((me ^ d) * chunk, 4), chunk), :].astype(BF16)
    w_copy.wait()


def attend_kernel(len_ref, *refs, ten, rows, prefix_rows, span_dev, heads_own, kv_own):
    packed, decoded = refs[:ten], refs[ten : 2 * ten]
    w_ref, ahead_ref = refs[2 * ten : 2 * ten + 2]
    keep_ref, send_ref, ahead_out, att, sem = refs[2 * ten + 2 :]
    copy = pltpu.make_async_copy(ahead_ref.at[0], ahead_out, sem)
    copy.start()
    me = lax.axis_index("ten")
    dec_dev = rows - span_dev
    pieces = heads_own // kv_own
    scale = HD ** (-0.5)
    order = bit_reversed(ten)
    keys = ten * (prefix_rows + rows)
    prefix_keys = ten * prefix_rows
    all_rows = ten * rows
    row = lax.broadcasted_iota(jnp.int32, (all_rows, 1), 0)
    col = lax.broadcasted_iota(jnp.int32, (1, keys), 1)
    row_pos = jnp.zeros((all_rows, 1), jnp.int32)
    prefix_pos = jnp.full((1, keys), 1 << 30, jnp.int32)
    fresh_pos = jnp.full((1, keys), 1 << 30, jnp.int32)
    for b, d in enumerate(order):
        t = me ^ d
        i = row - b * rows
        row_pos = jnp.where((i >= 0) & (i < rows), t * span_dev + i, row_pos)
        p = col - b * prefix_rows
        prefix_pos = jnp.where((p >= 0) & (p < prefix_rows), t * prefix_rows + p, prefix_pos)
        f = col - prefix_keys - b * rows
        fresh_pos = jnp.where((f >= 0) & (f < span_dev), t * span_dev + f, fresh_pos)
    visible = (prefix_pos < len_ref[0]) | (fresh_pos <= row_pos)
    bias = jnp.where(visible, 0.0, -1e30)
    bias = jnp.concatenate([bias] * pieces, axis=0)
    new_base = pieces * rows
    prefix_base = new_base + 2 * rows
    for g in range(kv_own):
        lanes = slice(g * HD, (g + 1) * HD)

        def gather(s):
            start = prefix_base + s * prefix_rows
            fresh = new_base + s * rows
            return jnp.concatenate(
                [packed[d][start : start + prefix_rows, lanes] for d in order]
                + [packed[d][fresh : fresh + rows, lanes] for d in order],
                axis=0,
            )

        heads = range(g * pieces, (g + 1) * pieces)
        q = jnp.concatenate(
            [
                packed[d][
                    (h // kv_own) * rows : (h // kv_own + 1) * rows,
                    (h % kv_own) * HD : (h % kv_own + 1) * HD,
                ]
                for h in heads
                for d in order
            ],
            axis=0,
        )
        scores = (
            lax.dot_general(q, gather(0), (((1,), (1,)), ((), ())), preferred_element_type=F32)
            * scale
            + bias
        )
        top = jnp.max(scores, axis=1, keepdims=True)
        exponent = jnp.exp(scores - top)
        total = jnp.sum(exponent, axis=1, keepdims=True)
        out = jnp.dot(exponent.astype(BF16), gather(1), preferred_element_type=F32) / total
        for n, h in enumerate(heads):
            att[:, h * HD : (h + 1) * HD] = out[n * all_rows : (n + 1) * all_rows]
            for b, d in enumerate(order):
                att[b * rows + span_dev : (b + 1) * rows, h * HD : (h + 1) * HD] = decoded[d][
                    h * dec_dev : (h + 1) * dec_dev, :
                ].astype(F32)
    half = all_rows // 2
    attended = att[...].astype(BF16)
    step = 512
    for n in range(0, w_ref.shape[1], step):
        part = jnp.dot(attended, w_ref[:, n : n + step], preferred_element_type=F32)
        keep_ref[:, n : n + step] = part[:half]
        send_ref[:, n : n + step] = part[half:].astype(BF16)
    copy.wait()


def route_kernel(*refs, parts, groups, local, rows):
    addends = refs[:parts]
    hidden_ref, gain_ref, router_ref, ids_ref, _ = refs[parts : parts + 5]
    residual_ref, map_ref = refs[parts + 5 : parts + 7]
    slot_refs = refs[parts + 7 :]
    me = lax.axis_index("exp")
    residual = hidden_ref[...].astype(F32)
    for a in addends:
        residual = residual + a[:rows, :].astype(F32)
    residual_ref[...] = residual
    width = residual.shape[1]
    mean_square = jnp.sum(residual * residual, axis=1, keepdims=True) / width
    normed = (residual * lax.rsqrt(mean_square + 1e-05) * gain_ref[...]).astype(BF16)
    logits = lax.dot_general(
        normed, router_ref[...], (((1,), (1,)), ((), ())), preferred_element_type=F32
    )
    diagonal = lax.broadcasted_iota(jnp.int32, (rows, rows), 0) == lax.broadcasted_iota(
        jnp.int32, (rows, rows), 1
    )
    first, second = (
        jnp.sum(jnp.where(diagonal, ids_ref[k : k + 1, :], 0), axis=1, keepdims=True)
        for k in range(2)
    )
    expert = lax.broadcasted_iota(jnp.int32, logits.shape, 1)
    first_logit = jnp.sum(jnp.where(expert == first, logits, 0.0), axis=1, keepdims=True)
    second_logit = jnp.sum(jnp.where(expert == second, logits, 0.0), axis=1, keepdims=True)
    top = jnp.maximum(first_logit, second_logit)
    first_exp, second_exp = jnp.exp(first_logit - top), jnp.exp(second_logit - top)
    total = first_exp + second_exp
    slots = local * groups * SLOTS
    lane = lax.broadcasted_iota(jnp.int32, (rows, slots), 1)
    within = lane % SLOTS
    group = lane // (SLOTS * local)
    slot_expert = (group ^ me) * local + (lane // SLOTS) % local
    is_first, is_second = slot_expert == first, slot_expert == second
    named = is_first | is_second
    below = (
        lax.broadcasted_iota(jnp.int32, (rows, rows), 1)
        < lax.broadcasted_iota(jnp.int32, (rows, rows), 0)
    )
    rank = jnp.dot(
        jnp.where(below, 1.0, 0.0).astype(BF16),
        jnp.where(named, 1.0, 0.0).astype(BF16),
        preferred_element_type=F32,
    )
    placed = named & (rank == within.astype(F32))
    map_ref[...] = jnp.where(
        placed, jnp.where(is_first, first_exp / total, second_exp / total), 0.0
    )
    chosen = lax.dot_general(
        jnp.where(placed, 1.0, 0.0).astype(BF16),
        normed,
        (((0,), (0,)), ((), ())),
        preferred_element_type=F32,
    ).astype(BF16)
    block = local * SLOTS
    for s, out in enumerate(slot_refs):
        out[...] = chosen[s * block : (s + 1) * block, :]


def hidden_kernel(*refs, pieces, expert, tile, resident, last):
    xs, gate_refs, refs = refs[:pieces], refs[pieces : pieces + 2], refs[pieces + 2 :]
    if resident:
        up_ref, refs = refs[0], refs[1:]
    else:
        up_low, up_hbm, down_hbm, refs = refs[0], refs[1], refs[2], refs[3:]
    if not last:
        next_gate, refs = refs[0], refs[1:]
    hidden_ref, refs = refs[0], refs[1:]
    if not resident:
        up_rest, down_low, refs = refs[0], refs[1], refs[2:]
    if not last:
        next_low, refs = refs[0], refs[1:]
    x_all, gates, sems = refs
    tiles = hidden_ref.shape[1] // tile
    stream, position = [], [0]
    if not resident:
        for i in range(tiles - 1):
            stream.append(
                (
                    up_hbm.at[expert, :, pl.ds((i + 1) * tile, tile)],
                    up_rest.at[:, pl.ds(i * tile, tile)],
                )
            )
        for i in range(down_low.shape[1] // tile):
            cols = pl.ds(i * tile, tile)
            stream.append((down_hbm.at[expert, :, cols], down_low.at[:, cols]))
    if not last:
        stream.append((next_gate.at[expert + 1, :, pl.ds(0, next_low.shape[1])], next_low))
    copies = [pltpu.make_async_copy(a, b, sems.at[i]) for i, (a, b) in enumerate(stream)]

    def advance(count):
        for copy in copies[position[0] : position[0] + count]:
            copy.start()
        position[0] = min(position[0] + count, len(copies))

    advance(3)
    for i, p in enumerate(xs):
        x_all[i * SLOTS : (i + 1) * SLOTS, :] = p[expert * SLOTS : (expert + 1) * SLOTS, :]
    first_width = gate_refs[0].shape[1]
    for i in range(tiles):
        start = i * tile
        if start < first_width:
            gate_tile = gate_refs[0][:, start : start + tile]
        else:
            gate_tile = gate_refs[1][:, start - first_width : start - first_width + tile]
        gate = jnp.dot(x_all[...], gate_tile, preferred_element_type=F32)
        gates[:, start : start + tile] = gate / (1.0 + jnp.exp(-gate))
    for i in range(tiles):
        cols = slice(i * tile, (i + 1) * tile)
        if resident:
            up_tile = up_ref[:, cols]
        elif i == 0:
            up_tile = up_low[...]
        else:
            copies[i - 1].wait()
            advance(1)
            up_tile = up_rest[:, (i - 1) * tile : i * tile]
        up = jnp.dot(x_all[...], up_tile, preferred_element_type=F32)
        hidden_ref[:, cols] = (gates[:, cols] * up).astype(BF16)
    advance(len(copies))
    for copy in copies[0 if resident else tiles - 1 :]:
        copy.wait()


def down_kernel(hidden_ref, down_ref, *refs, resident, last, expert, tile, extra):
    if not resident:
        down_hbm, refs = refs[0], refs[1 + extra :]
    if not last:
        next_gate, next_up, refs = refs[0], refs[1], refs[2:]
    keep_ref, send_ref, refs = refs[0], refs[1], refs[2:]
    if not resident:
        rest_ref, refs = refs[0], refs[1:]
    if not last:
        gate_high, up_low, refs = refs[0], refs[1], refs[2:]
    sems = refs[0]
    split = down_ref.shape[1]
    half, width = keep_ref.shape
    pending = []
    if not last:
        low = next_gate.shape[2] - tile
        pending = load_all(
            (
                (next_gate.at[expert + 1, :, pl.ds(low, tile)], gate_high),
                (next_up.at[expert + 1, :, pl.ds(0, tile)], up_low),
            ),
            sems,
        )
    copies = []
    if not resident:
        for i in range((width - split) // tile):
            copies.append(
                pltpu.make_async_copy(
                    down_hbm.at[expert, :, pl.ds(split + i * tile, tile)],
                    rest_ref.at[:, pl.ds(i * tile, tile)],
                    sems.at[2 + i],
                )
            )
        for copy in copies[:3]:
            copy.start()
    for start in range(0, width, tile):
        cols = slice(start, start + tile)
        if start >= split:
            i = (start - split) // tile
            copies[i].wait()
            for copy in copies[i + 3 : i + 4]:
                copy.start()
            down_tile = rest_ref[:, i * tile : (i + 1) * tile]
        else:
            down_tile = down_ref[:, cols]
        part = jnp.dot(hidden_ref[...], down_tile, preferred_element_type=F32)
        keep_ref[:, cols] = part[:half]
        send_ref[:, cols] = part[half:].astype(BF16)
    for copy in pending:
        copy.wait()


def add_kernel(*refs, parts, firsts, rows, skip=0):
    addends, outs = refs[:parts], refs[parts + skip :]
    total = addends[0][firsts[0] : firsts[0] + rows, :].astype(F32)
    for a, first in zip(addends[1:], firsts[1:]):
        total = total + a[first : first + rows, :].astype(F32)
    each = outs[0].shape[0]
    for i, out in enumerate(outs):
        out[...] = total[i * each : (i + 1) * each, :].astype(out.dtype)


def mix_kernel(residual_ref, map_ref, *refs, local, groups):
    returned, out = refs[:-1], refs[-1]
    rows = residual_ref.shape[0]
    table = jnp.concatenate(
        [returned[e * groups + d][...] for d in range(groups) for e in range(local)], axis=0
    )
    weights = map_ref[...]
    high = weights.astype(BF16)
    rest = weights - high.astype(F32)
    middle = rest.astype(BF16)
    low = (rest - middle.astype(F32)).astype(BF16)
    stacked = jnp.concatenate([high, middle, low], axis=0)
    mixed = jnp.dot(stacked, table, preferred_element_type=F32)
    total = mixed[:rows] + mixed[rows : 2 * rows] + mixed[2 * rows :]
    out[...] = (residual_ref[...] + total).astype(out.dtype)


def fetch_kernel(source_ref, _, out_ref, token_ref, sem, *, expert, first):
    source = source_ref if expert is None else source_ref.at[expert]
    copy = pltpu.make_async_copy(source.at[:, pl.ds(first, out_ref.shape[1])], out_ref, sem)
    copy.start()
    token_ref[...] = jnp.zeros_like(token_ref)
    copy.wait()


def fetch(source, expert, after, columns=None, first=0):
    rows, width = source.shape[-2:]
    return call(
        functools.partial(fetch_kernel, expert=expert, first=first),
        (source, after),
        [HBM, VMEM],
        [out((rows, columns or width), BF16), out((8, HD), F32)],
        [pltpu.SemaphoreType.DMA],
        limit=2,
    )


def send_to(x, axis, distance):
    return lax.ppermute(x, axis, xor_pairs(lax.axis_size(axis), distance))


def halves_down(keep, send, axis, size, cuts=1):
    addends = [keep]
    rows = keep.shape[0]
    for bit in up_bits(size)[:-1]:
        addends.append(send_to(send, axis, bit))
        rows //= 2
        parts = cuts if bit * 4 == size else 1
        sends = call(
            functools.partial(
                add_kernel, firsts=[rows] * len(addends), rows=rows, parts=len(addends)
            ),
            addends,
            [VMEM] * len(addends),
            [out((rows // parts, keep.shape[1]), BF16)] * parts,
            limit=3,
        )
        send = sends[0]
    share = rows // cuts
    result = []
    for c in reversed(range(cuts)):
        got = send_to(sends[c], axis, size // 2)
        result.append([(a, c * share) for a in addends] + [(got, 0)])
    return result[::-1], share, sends[-1]


def on_device(
    hidden_in,
    queries,
    new_kv,
    prefix_kv,
    decode_kv,
    prefix_len,
    decode_len,
    out_proj,
    norm_gain,
    router_w,
    expert_ids,
    w_gate,
    w_up,
    w_down,
):
    ten = lax.axis_size("ten")
    groups = lax.axis_size("exp")
    rows, width = hidden_in.shape
    dec_dev = decode_len.shape[0]
    span_dev = rows - dec_dev
    heads_q = queries.shape[1] // HD
    heads_kv = new_kv.shape[2] // HD
    per_kv = heads_q // heads_kv
    heads_own = heads_q // ten
    kv_own = max(1, heads_own // per_kv)
    prefix_rows = prefix_kv.shape[2]
    experts = router_w.shape[1]
    local = experts // groups

    packed_rows = (heads_own // kv_own) * rows + 2 * rows + 2 * prefix_rows
    packed = call(
        functools.partial(pack_kernel, heads_own=heads_own, per_kv=per_kv, kv_own=kv_own),
        (queries, new_kv, prefix_kv),
        [HBM] * 3,
        [out((packed_rows, kv_own * HD), BF16)] * ten,
        [pltpu.VMEM(a.shape, BF16) for a in (queries, new_kv, prefix_kv)]
        + [pltpu.SemaphoreType.DMA((3,))],
    )
    packed = [packed[0]] + [
        lax.ppermute(packed[d], "ten", xor_pairs(ten, d)) for d in range(1, ten)
    ]

    q_block = -(-dec_dev // 8) * 8
    *decoded, proj = call(
        functools.partial(decode_kernel, per_kv=per_kv, span_dev=span_dev, block=q_block),
        (decode_len, queries, decode_kv, new_kv, out_proj),
        [HBM] * 5,
        [out((heads_own * dec_dev, HD), BF16)] * ten + [out(out_proj.shape, BF16)],
        [
            pltpu.SMEM(decode_len.shape, jnp.int32),
            pltpu.VMEM((q_block, queries.shape[1]), BF16),
            pltpu.VMEM(decode_kv.shape, BF16),
            pltpu.VMEM(new_kv.shape, BF16),
            pltpu.VMEM((heads_q * dec_dev, HD), F32),
            pltpu.VMEM((heads_q * dec_dev, HD), F32),
            pltpu.SemaphoreType.DMA((5,)),
        ],
        limit=5,
    )
    decoded = [decoded[0]] + [
        lax.ppermute(decoded[d], "ten", xor_pairs(ten, d)) for d in range(1, ten)
    ]
    half = ten * rows // 2
    keep, send, up = call(
        functools.partial(
            attend_kernel,
            ten=ten,
            rows=rows,
            prefix_rows=prefix_rows,
            span_dev=span_dev,
            heads_own=heads_own,
            kv_own=kv_own,
        ),
        (prefix_len, *packed, *decoded, held(proj), w_up),
        [SMEM] + [VMEM] * (2 * ten) + [VMEM, HBM],
        [
            out((half, width), F32),
            out((half, width), BF16),
            out(w_up.shape[1:], BF16),
        ],
        [pltpu.VMEM((ten * rows, heads_own * HD), F32), pltpu.SemaphoreType.DMA],
        limit=4,
    )
    (addends,), _, last_sent = halves_down(keep, send, "ten", ten)
    addends = [a for a, _ in addends]
    down, down_token = fetch(w_down, 0, last_sent)

    routed = call(
        functools.partial(
            route_kernel, parts=len(addends), groups=groups, local=local, rows=rows
        ),
        (
            *addends,
            hidden_in,
            norm_gain.reshape(1, width),
            router_w.T,
            expert_ids.T,
            down_token,
        ),
        [VMEM] * (len(addends) + 5),
        [out((rows, width), F32), out((rows, experts * SLOTS), F32)]
        + [out((local * SLOTS, width), BF16)] * groups,
        limit=3,
    )
    residual, weight_map, slots = routed[0], routed[1], routed[2:]

    block = [slots[0]] + [send_to(slots[d], "exp", d) for d in range(1, groups)]
    for bit in reversed(up_bits(ten)):
        block = block + [send_to(b, "ten", bit) for b in block]

    hidden_units = w_gate.shape[2]
    gate_half = hidden_units // 2
    gate_a, gate_token = fetch(w_gate, 0, slots[0], gate_half)
    gate_b, _ = fetch(w_gate, 0, gate_token, gate_half, gate_half)
    tile = min(512, hidden_units // 4)
    tiles = hidden_units // tile
    down_low_width = 2 * tile
    half = len(block) * SLOTS // 2
    returned = []
    for e in range(local):
        last, resident = e == local - 1, e == 0
        args, specs = [*block], [VMEM] * len(block)
        outs = [out((2 * half, hidden_units), BF16)]
        if resident:
            args += [held(gate_a), held(gate_b), held(up)]
            specs += [VMEM] * 3
        else:
            args += [held(next_low), held(gate_high), held(up_low), w_up, w_down]
            specs += [VMEM] * 3 + [HBM] * 2
            outs += [
                out((width, hidden_units - tile), BF16),
                out((hidden_units, down_low_width), BF16),
            ]
        if not last:
            args.append(w_gate)
            specs.append(HBM)
            outs.append(out((width, hidden_units - tile), BF16))
        hidden, *rest = call(
            functools.partial(
                hidden_kernel,
                pieces=len(block),
                expert=e,
                tile=tile,
                resident=resident,
                last=last,
            ),
            args,
            specs,
            outs,
            [
                pltpu.VMEM((2 * half, width), BF16),
                pltpu.VMEM((2 * half, hidden_units), F32),
                pltpu.SemaphoreType.DMA((tiles + 4,)),
            ],
            limit=3,
            flops=8 * half * width * hidden_units,
        )
        if not last:
            next_low = rest[-1]
        args, specs = [hidden], [VMEM]
        outs = [out((half, width), F32), out((half, width), BF16)]
        if resident:
            args.append(held(down))
            specs.append(VMEM)
        else:
            args += [held(rest[1]), w_down, rest[0], before]
            specs += [VMEM, HBM, VMEM, VMEM]
            outs.append(out((hidden_units, width - down_low_width), BF16))
        if not last:
            args += [w_gate, w_up]
            specs += [HBM, HBM]
            outs += [out((width, tile), BF16)] * 2
        keep, send, *rest = call(
            functools.partial(
                down_kernel, resident=resident, last=last, expert=e, tile=tile, extra=2
            ),
            args,
            specs,
            outs,
            [pltpu.SemaphoreType.DMA((2 + width // tile,))],
            limit=3,
            flops=4 * half * width * hidden_units,
        )
        if not last:
            gate_high, up_low = rest[-2:]
            rest = rest[:-2]
        cuts = 2 if groups > 2 else 1
        shares, share, before = halves_down(keep, send, "ten", ten, cuts)
        mine = [None] * groups
        each = groups // cuts
        for c in reversed(range(cuts)):
            addends = [a for a, _ in shares[c]]
            unused = rest if c == 0 else []
            pieces = call(
                functools.partial(
                    add_kernel,
                    parts=len(addends),
                    firsts=[first for _, first in shares[c]],
                    rows=share,
                    skip=len(unused),
                ),
                (*addends, *unused),
                [VMEM] * (len(addends) + len(unused)),
                [out((SLOTS, width), BF16)] * each,
                limit=3,
            )
            for i in reversed(range(each)):
                d = c * each + i
                mine[d] = send_to(pieces[i], "exp", d) if d else pieces[i]
        returned += mine
    return pl.pallas_call(
        functools.partial(mix_kernel, local=local, groups=groups),
        in_specs=[VMEM] * (2 + len(returned)),
        out_specs=VMEM,
        out_shape=jax.ShapeDtypeStruct((rows, width), BF16),
        compiler_params=pltpu.CompilerParams(vmem_limit_bytes=16 * MIB),
        name="mix",
    )(residual, weight_map, *returned)


def solution(mesh):
    in_specs = (
        P(("rep", "exp", "ten"), None),
        P(("rep", "exp", "ten"), None),
        P(None, ("rep", "exp", "ten"), None),
        P(None, ("rep", "exp"), "ten", None),
        P(None, ("rep", "exp", "ten"), None, None),
        P(("rep", "exp")),
        P(("rep", "exp", "ten")),
        P("ten", None),
        P(),
        P(),
        P(("rep", "exp", "ten"), None),
        P("exp", None, "ten"),
        P("exp", None, "ten"),
        P("exp", "ten", None),
    )
    out_specs = P(("rep", "exp", "ten"), None)

    return jax.shard_map(
        on_device, mesh=mesh, in_specs=in_specs, out_specs=out_specs, check_vma=False
    )
```

```python
import functools

import jax
import jax.numpy as jnp
from jax import lax
from jax.experimental import pallas as pl
from jax.experimental.pallas import tpu as pltpu
from jax.sharding import PartitionSpec as P

HD = 128
SLOTS = 8
F32 = jnp.float32
BF16 = jnp.bfloat16
MIB = 2**20
VMEM = pl.BlockSpec(memory_space=pltpu.VMEM)
SMEM = pl.BlockSpec(memory_space=pltpu.SMEM)
HBM = pl.BlockSpec(memory_space=pltpu.HBM)


def xor_pairs(size, distance):
    return [(i, i ^ distance) for i in range(size)]


def bit_reversed(size):
    order = [0]
    step = size // 2
    while step:
        order = order + [o + step for o in order]
        step //= 2
    return order


def up_bits(size):
    return [1 << b for b in range(size.bit_length() - 1)]


def out(shape, dtype):
    return jax.ShapeDtypeStruct(shape, dtype)


def held(array):
    return pltpu.with_memory_space_constraint(array, pltpu.VMEM)


def call(kernel, args, specs, outs, scratch=(), limit=4, flops=0, aliases=None):
    limit *= max(1, lax.axis_size("ten") * lax.axis_size("exp") // 16)
    args = [
        pltpu.with_memory_space_constraint(a, pltpu.HBM) if s is HBM else a
        for a, s in zip(args, specs)
    ]
    return pl.pallas_call(
        kernel,
        in_specs=specs,
        out_specs=[VMEM] * len(outs),
        out_shape=outs,
        scratch_shapes=list(scratch),
        compiler_params=pltpu.CompilerParams(vmem_limit_bytes=limit * MIB),
        cost_estimate=pl.CostEstimate(flops=flops, bytes_accessed=0, transcendentals=0),
        input_output_aliases=aliases or {},
    )(*args)


def load_all(pairs, sems):
    copies = [pltpu.make_async_copy(a, b, sems.at[i]) for i, (a, b) in enumerate(pairs)]
    for copy in copies:
        copy.start()
    return copies


def pack_kernel(q_hbm, new_hbm, prefix_hbm, *refs, heads_own, per_kv, kv_own):
    out_refs, (q_ref, new_ref, prefix_ref, sems) = refs[:-4], refs[-4:]
    pairs = ((q_hbm, q_ref), (new_hbm, new_ref), (prefix_hbm, prefix_ref))
    for copy in load_all(pairs, sems):
        copy.wait()
    me = lax.axis_index("ten")
    rows = q_ref.shape[0]
    prefix_rows = prefix_ref.shape[2]
    width = kv_own * HD
    pieces = heads_own // kv_own
    for d, out in enumerate(out_refs):
        t = me ^ d
        q_start = pl.multiple_of(t * (heads_own * HD), HD)
        for j in range(pieces):
            out[j * rows : (j + 1) * rows, :] = q_ref[
                :, pl.ds(pl.multiple_of(q_start + j * width, HD), width)
            ]
        kv_start = pl.multiple_of(((t * heads_own) // per_kv) * HD, HD)
        base = pieces * rows
        for s in range(2):
            out[base : base + rows, :] = new_ref[s, :, pl.ds(kv_start, width)]
            base += rows
        for s in range(2):
            out[base : base + prefix_rows, :] = prefix_ref[s, 0, :, pl.ds(kv_start, width)]
            base += prefix_rows


def decode_kernel(len_hbm, q_hbm, kv_hbm, new_hbm, w_hbm, *refs, per_kv, span_dev, block):
    out_refs, (w_low, len_ref, q_ref, kv_ref, new_ref, q_heads, scratch, sems) = refs[:-8], refs[-8:]
    q_rows = q_hbm.at[pl.ds(q_hbm.shape[0] - block, block)]
    pairs = ((len_hbm, len_ref), (q_rows, q_ref), (kv_hbm, kv_ref), (new_hbm, new_ref))
    loads = load_all(pairs, sems)
    w_copy = pltpu.make_async_copy(
        w_hbm.at[:, pl.ds(0, w_low.shape[1])], w_low, sems.at[len(pairs)]
    )
    w_copy.start()
    for copy in loads:
        copy.wait()
    me = lax.axis_index("ten")
    dec_dev, ctx_len, kv_width = kv_ref.shape[1:]
    heads = q_ref.shape[1] // HD
    heads_kv = kv_width // HD
    for h in range(heads):
        q_heads[h * dec_dev : (h + 1) * dec_dev, :] = q_ref[
            block - dec_dev :, h * HD : (h + 1) * HD
        ].astype(F32)
    scale = HD ** (-0.5)
    row_group = lax.broadcasted_iota(jnp.int32, (heads, kv_width), 0) // per_kv
    lane_group = lax.broadcasted_iota(jnp.int32, (heads, kv_width), 1) // HD
    own = row_group == lane_group
    position = lax.broadcasted_iota(jnp.int32, (heads, ctx_len), 1)
    for r in range(dec_dev):
        q = q_heads[pl.ds(r, heads, stride=dec_dev), :].astype(BF16)
        wide = jnp.where(own, jnp.concatenate([q] * heads_kv, axis=1), jnp.zeros((), BF16))
        scores = (
            lax.dot_general(
                wide, kv_ref[0, r], (((1,), (1,)), ((), ())), preferred_element_type=F32
            )
            * scale
        )
        new_key = new_ref[0, span_dev + r : span_dev + r + 1, :].astype(F32)
        new_value = new_ref[1, span_dev + r : span_dev + r + 1, :].astype(F32)
        new_score = jnp.sum(wide.astype(F32) * new_key, axis=1, keepdims=True) * scale
        visible = position < len_ref[r]
        masked = jnp.where(visible, scores, -1e30)
        top = jnp.maximum(jnp.max(masked, axis=1, keepdims=True), new_score)
        exponent = jnp.where(visible, jnp.exp(masked - top), 0.0)
        new_exponent = jnp.exp(new_score - top)
        total = jnp.sum(exponent, axis=1, keepdims=True) + new_exponent
        mixed = jnp.dot(exponent.astype(BF16), kv_ref[1, r], preferred_element_type=F32)
        mixed = mixed + new_exponent.astype(BF16).astype(F32) * new_value
        mixed = jnp.where(own, mixed, 0.0)
        picked = mixed[:, :HD]
        for g in range(1, heads_kv):
            picked = picked + mixed[:, g * HD : (g + 1) * HD]
        scratch[pl.ds(r, heads, stride=dec_dev), :] = picked / total
    chunk = scratch.shape[0] // len(out_refs)
    for d, out in enumerate(out_refs):
        out[...] = scratch[pl.ds(pl.multiple_of((me ^ d) * chunk, 4), chunk), :].astype(BF16)
    w_copy.wait()


def attend_kernel(len_ref, *refs, ten, rows, prefix_rows, span_dev, heads_own, kv_own):
    packed, decoded = refs[:ten], refs[ten : 2 * ten]
    w_ref, ahead_ref = refs[2 * ten : 2 * ten + 2]
    keep_ref, send_ref, ahead_out, att, sem = refs[2 * ten + 2 :]
    copy = pltpu.make_async_copy(ahead_ref.at[0], ahead_out, sem)
    copy.start()
    me = lax.axis_index("ten")
    dec_dev = rows - span_dev
    pieces = heads_own // kv_own
    scale = HD ** (-0.5)
    order = bit_reversed(ten)
    keys = ten * (prefix_rows + rows)
    prefix_keys = ten * prefix_rows
    all_rows = ten * rows
    row = lax.broadcasted_iota(jnp.int32, (all_rows, 1), 0)
    col = lax.broadcasted_iota(jnp.int32, (1, keys), 1)
    row_pos = jnp.zeros((all_rows, 1), jnp.int32)
    prefix_pos = jnp.full((1, keys), 1 << 30, jnp.int32)
    fresh_pos = jnp.full((1, keys), 1 << 30, jnp.int32)
    for b, d in enumerate(order):
        t = me ^ d
        i = row - b * rows
        row_pos = jnp.where((i >= 0) & (i < rows), t * span_dev + i, row_pos)
        p = col - b * prefix_rows
        prefix_pos = jnp.where((p >= 0) & (p < prefix_rows), t * prefix_rows + p, prefix_pos)
        f = col - prefix_keys - b * rows
        fresh_pos = jnp.where((f >= 0) & (f < span_dev), t * span_dev + f, fresh_pos)
    visible = (prefix_pos < len_ref[0]) | (fresh_pos <= row_pos)
    bias = jnp.where(visible, 0.0, -1e30)
    bias = jnp.concatenate([bias] * pieces, axis=0)
    new_base = pieces * rows
    prefix_base = new_base + 2 * rows
    for g in range(kv_own):
        lanes = slice(g * HD, (g + 1) * HD)

        def gather(s):
            start = prefix_base + s * prefix_rows
            fresh = new_base + s * rows
            return jnp.concatenate(
                [packed[d][start : start + prefix_rows, lanes] for d in order]
                + [packed[d][fresh : fresh + rows, lanes] for d in order],
                axis=0,
            )

        heads = range(g * pieces, (g + 1) * pieces)
        q = jnp.concatenate(
            [
                packed[d][
                    (h // kv_own) * rows : (h // kv_own + 1) * rows,
                    (h % kv_own) * HD : (h % kv_own + 1) * HD,
                ]
                for h in heads
                for d in order
            ],
            axis=0,
        )
        scores = (
            lax.dot_general(q, gather(0), (((1,), (1,)), ((), ())), preferred_element_type=F32)
            * scale
            + bias
        )
        top = jnp.max(scores, axis=1, keepdims=True)
        exponent = jnp.exp(scores - top)
        total = jnp.sum(exponent, axis=1, keepdims=True)
        out = jnp.dot(exponent.astype(BF16), gather(1), preferred_element_type=F32) / total
        for n, h in enumerate(heads):
            att[:, h * HD : (h + 1) * HD] = out[n * all_rows : (n + 1) * all_rows]
            for b, d in enumerate(order):
                att[b * rows + span_dev : (b + 1) * rows, h * HD : (h + 1) * HD] = decoded[d][
                    h * dec_dev : (h + 1) * dec_dev, :
                ].astype(F32)
    half = all_rows // 2
    attended = att[...].astype(BF16)
    step = 512
    for n in range(0, w_ref.shape[1], step):
        part = jnp.dot(attended, w_ref[:, n : n + step], preferred_element_type=F32)
        keep_ref[:, n : n + step] = part[:half]
        send_ref[:, n : n + step] = part[half:].astype(BF16)
    copy.wait()


def route_kernel(*refs, parts, groups, local, rows):
    addends = refs[:parts]
    hidden_ref, gain_ref, router_ref, ids_ref, _ = refs[parts : parts + 5]
    residual_ref, map_ref = refs[parts + 5 : parts + 7]
    slot_refs = refs[parts + 7 :]
    me = lax.axis_index("exp")
    residual = hidden_ref[...].astype(F32)
    for a in addends:
        residual = residual + a[:rows, :].astype(F32)
    residual_ref[...] = residual
    width = residual.shape[1]
    mean_square = jnp.sum(residual * residual, axis=1, keepdims=True) / width
    normed = (residual * lax.rsqrt(mean_square + 1e-05) * gain_ref[...]).astype(BF16)
    logits = lax.dot_general(
        normed, router_ref[...], (((1,), (1,)), ((), ())), preferred_element_type=F32
    )
    diagonal = lax.broadcasted_iota(jnp.int32, (rows, rows), 0) == lax.broadcasted_iota(
        jnp.int32, (rows, rows), 1
    )
    first, second = (
        jnp.sum(jnp.where(diagonal, ids_ref[k : k + 1, :], 0), axis=1, keepdims=True)
        for k in range(2)
    )
    expert = lax.broadcasted_iota(jnp.int32, logits.shape, 1)
    first_logit = jnp.sum(jnp.where(expert == first, logits, 0.0), axis=1, keepdims=True)
    second_logit = jnp.sum(jnp.where(expert == second, logits, 0.0), axis=1, keepdims=True)
    top = jnp.maximum(first_logit, second_logit)
    first_exp, second_exp = jnp.exp(first_logit - top), jnp.exp(second_logit - top)
    total = first_exp + second_exp
    slots = local * groups * SLOTS
    lane = lax.broadcasted_iota(jnp.int32, (rows, slots), 1)
    within = lane % SLOTS
    group = lane // (SLOTS * local)
    slot_expert = (group ^ me) * local + (lane // SLOTS) % local
    is_first, is_second = slot_expert == first, slot_expert == second
    named = is_first | is_second
    below = (
        lax.broadcasted_iota(jnp.int32, (rows, rows), 1)
        < lax.broadcasted_iota(jnp.int32, (rows, rows), 0)
    )
    rank = jnp.dot(
        jnp.where(below, 1.0, 0.0).astype(BF16),
        jnp.where(named, 1.0, 0.0).astype(BF16),
        preferred_element_type=F32,
    )
    placed = named & (rank == within.astype(F32))
    map_ref[...] = jnp.where(
        placed, jnp.where(is_first, first_exp / total, second_exp / total), 0.0
    )
    chosen = lax.dot_general(
        jnp.where(placed, 1.0, 0.0).astype(BF16),
        normed,
        (((0,), (0,)), ((), ())),
        preferred_element_type=F32,
    ).astype(BF16)
    block = local * SLOTS
    for s, out in enumerate(slot_refs):
        out[...] = chosen[s * block : (s + 1) * block, :]


def hidden_kernel(*refs, pieces, expert, tile, resident, last):
    xs, gate_refs, refs = refs[:pieces], refs[pieces : pieces + 2], refs[pieces + 2 :]
    if resident:
        up_ref, refs = refs[0], refs[1:]
    else:
        up_low, up_hbm, down_hbm, refs = refs[0], refs[1], refs[2], refs[3:]
    if not last:
        next_gate, refs = refs[0], refs[1:]
    hidden_ref, refs = refs[0], refs[1:]
    if not resident:
        up_rest, down_low, refs = refs[0], refs[1], refs[2:]
    if not last:
        next_low, refs = refs[0], refs[1:]
    x_all, gates, sems = refs
    tiles = hidden_ref.shape[1] // tile
    stream, position = [], [0]
    if not resident:
        for i in range(tiles - 1):
            stream.append(
                (
                    up_hbm.at[expert, :, pl.ds((i + 1) * tile, tile)],
                    up_rest.at[:, pl.ds(i * tile, tile)],
                )
            )
        for i in range(down_low.shape[1] // tile):
            cols = pl.ds(i * tile, tile)
            stream.append((down_hbm.at[expert, :, cols], down_low.at[:, cols]))
    if not last:
        stream.append((next_gate.at[expert + 1, :, pl.ds(0, next_low.shape[1])], next_low))
    copies = [pltpu.make_async_copy(a, b, sems.at[i]) for i, (a, b) in enumerate(stream)]

    def advance(count):
        for copy in copies[position[0] : position[0] + count]:
            copy.start()
        position[0] = min(position[0] + count, len(copies))

    advance(3)
    for i, p in enumerate(xs):
        x_all[i * SLOTS : (i + 1) * SLOTS, :] = p[expert * SLOTS : (expert + 1) * SLOTS, :]
    first_width = gate_refs[0].shape[1]
    for i in range(tiles):
        start = i * tile
        if start < first_width:
            gate_tile = gate_refs[0][:, start : start + tile]
        else:
            gate_tile = gate_refs[1][:, start - first_width : start - first_width + tile]
        gate = jnp.dot(x_all[...], gate_tile, preferred_element_type=F32)
        gate = gate / (1.0 + jnp.exp(-gate))
        if resident:
            up_tile = up_ref[:, start : start + tile]
            up = jnp.dot(x_all[...], up_tile, preferred_element_type=F32)
            hidden_ref[:, start : start + tile] = (gate * up).astype(BF16)
        else:
            gates[:, start : start + tile] = gate
    for i in range(0 if resident else tiles):
        cols = slice(i * tile, (i + 1) * tile)
        if i == 0:
            up_tile = up_low[...]
        else:
            copies[i - 1].wait()
            advance(1)
            up_tile = up_rest[:, (i - 1) * tile : i * tile]
        up = jnp.dot(x_all[...], up_tile, preferred_element_type=F32)
        hidden_ref[:, cols] = (gates[:, cols] * up).astype(BF16)
    advance(len(copies))
    for copy in copies[0 if resident else tiles - 1 :]:
        copy.wait()


def down_kernel(hidden_ref, down_ref, *refs, resident, last, expert, tile, extra):
    if not resident:
        down_hbm, refs = refs[0], refs[1 + extra :]
    if not last:
        next_gate, next_up, refs = refs[0], refs[1], refs[2:]
    keep_ref, send_ref, refs = refs[0], refs[1], refs[2:]
    if not resident:
        rest_ref, refs = refs[0], refs[1:]
    if not last:
        gate_high, up_low, refs = refs[0], refs[1], refs[2:]
    sems = refs[0]
    split = down_ref.shape[1]
    half, width = keep_ref.shape
    pending = []
    if not last:
        low = next_gate.shape[2] - tile
        pending = load_all(
            (
                (next_gate.at[expert + 1, :, pl.ds(low, tile)], gate_high),
                (next_up.at[expert + 1, :, pl.ds(0, tile)], up_low),
            ),
            sems,
        )
    copies = []
    if not resident:
        for i in range((width - split) // tile):
            copies.append(
                pltpu.make_async_copy(
                    down_hbm.at[expert, :, pl.ds(split + i * tile, tile)],
                    rest_ref.at[:, pl.ds(i * tile, tile)],
                    sems.at[2 + i],
                )
            )
        for copy in copies[:4]:
            copy.start()
    for start in range(0, width, tile):
        cols = slice(start, start + tile)
        if start >= split:
            i = (start - split) // tile
            copies[i].wait()
            for copy in copies[i + 4 : i + 5]:
                copy.start()
            down_tile = rest_ref[:, i * tile : (i + 1) * tile]
        else:
            down_tile = down_ref[:, cols]
        part = jnp.dot(hidden_ref[...], down_tile, preferred_element_type=F32)
        keep_ref[:, cols] = part[:half]
        send_ref[:, cols] = part[half:].astype(BF16)
    for copy in pending:
        copy.wait()


def add_kernel(*refs, parts, firsts, rows, skip=0):
    addends, outs = refs[:parts], refs[parts + skip :]
    total = addends[0][firsts[0] : firsts[0] + rows, :].astype(F32)
    for a, first in zip(addends[1:], firsts[1:]):
        total = total + a[first : first + rows, :].astype(F32)
    each = outs[0].shape[0]
    for i, out in enumerate(outs):
        out[...] = total[i * each : (i + 1) * each, :].astype(out.dtype)


def mix_kernel(residual_ref, map_ref, *refs, local, groups):
    returned, out = refs[:-1], refs[-1]
    rows = residual_ref.shape[0]
    table = jnp.concatenate(
        [returned[e * groups + d][...] for d in range(groups) for e in range(local)], axis=0
    )
    weights = map_ref[...]
    high = weights.astype(BF16)
    rest = weights - high.astype(F32)
    middle = rest.astype(BF16)
    low = (rest - middle.astype(F32)).astype(BF16)
    stacked = jnp.concatenate([high, middle, low], axis=0)
    mixed = jnp.dot(stacked, table, preferred_element_type=F32)
    total = mixed[:rows] + mixed[rows : 2 * rows] + mixed[2 * rows :]
    out[...] = (residual_ref[...] + total).astype(out.dtype)


def fetch_kernel(source_ref, _, out_ref, token_ref, sem, *, expert, first):
    source = source_ref if expert is None else source_ref.at[expert]
    copy = pltpu.make_async_copy(source.at[:, pl.ds(first, out_ref.shape[1])], out_ref, sem)
    copy.start()
    token_ref[...] = jnp.zeros_like(token_ref)
    copy.wait()


def fetch(source, expert, after, columns=None, first=0):
    rows, width = source.shape[-2:]
    return call(
        functools.partial(fetch_kernel, expert=expert, first=first),
        (source, after),
        [HBM, VMEM],
        [out((rows, columns or width), BF16), out((8, HD), F32)],
        [pltpu.SemaphoreType.DMA],
        limit=2,
    )


def send_to(x, axis, distance):
    return lax.ppermute(x, axis, xor_pairs(lax.axis_size(axis), distance))


def halves_down(keep, send, axis, size, cuts=1):
    addends = [keep]
    rows = keep.shape[0]
    for bit in up_bits(size)[:-1]:
        addends.append(send_to(send, axis, bit))
        rows //= 2
        parts = cuts if bit * 4 == size else 1
        sends = call(
            functools.partial(
                add_kernel, firsts=[rows] * len(addends), rows=rows, parts=len(addends)
            ),
            addends,
            [VMEM] * len(addends),
            [out((rows // parts, keep.shape[1]), BF16)] * parts,
            limit=3,
        )
        send = sends[0]
    share = rows // cuts
    result = []
    for c in reversed(range(cuts)):
        got = send_to(sends[c], axis, size // 2)
        result.append([(a, c * share) for a in addends] + [(got, 0)])
    return result[::-1], share, sends[-1]


def on_device(
    hidden_in,
    queries,
    new_kv,
    prefix_kv,
    decode_kv,
    prefix_len,
    decode_len,
    out_proj,
    norm_gain,
    router_w,
    expert_ids,
    w_gate,
    w_up,
    w_down,
):
    ten = lax.axis_size("ten")
    groups = lax.axis_size("exp")
    rows, width = hidden_in.shape
    dec_dev = decode_len.shape[0]
    span_dev = rows - dec_dev
    heads_q = queries.shape[1] // HD
    heads_kv = new_kv.shape[2] // HD
    per_kv = heads_q // heads_kv
    heads_own = heads_q // ten
    kv_own = max(1, heads_own // per_kv)
    prefix_rows = prefix_kv.shape[2]
    experts = router_w.shape[1]
    local = experts // groups

    packed_rows = (heads_own // kv_own) * rows + 2 * rows + 2 * prefix_rows
    packed = call(
        functools.partial(pack_kernel, heads_own=heads_own, per_kv=per_kv, kv_own=kv_own),
        (queries, new_kv, prefix_kv),
        [HBM] * 3,
        [out((packed_rows, kv_own * HD), BF16)] * ten,
        [pltpu.VMEM(a.shape, BF16) for a in (queries, new_kv, prefix_kv)]
        + [pltpu.SemaphoreType.DMA((3,))],
    )
    packed = [packed[0]] + [
        lax.ppermute(packed[d], "ten", xor_pairs(ten, d)) for d in range(1, ten)
    ]

    q_block = -(-dec_dev // 8) * 8
    *decoded, proj = call(
        functools.partial(decode_kernel, per_kv=per_kv, span_dev=span_dev, block=q_block),
        (decode_len, queries, decode_kv, new_kv, out_proj),
        [HBM] * 5,
        [out((heads_own * dec_dev, HD), BF16)] * ten + [out(out_proj.shape, BF16)],
        [
            pltpu.SMEM(decode_len.shape, jnp.int32),
            pltpu.VMEM((q_block, queries.shape[1]), BF16),
            pltpu.VMEM(decode_kv.shape, BF16),
            pltpu.VMEM(new_kv.shape, BF16),
            pltpu.VMEM((heads_q * dec_dev, HD), F32),
            pltpu.VMEM((heads_q * dec_dev, HD), F32),
            pltpu.SemaphoreType.DMA((5,)),
        ],
        limit=5,
    )
    decoded = [decoded[0]] + [
        lax.ppermute(decoded[d], "ten", xor_pairs(ten, d)) for d in range(1, ten)
    ]
    half = ten * rows // 2
    keep, send, up = call(
        functools.partial(
            attend_kernel,
            ten=ten,
            rows=rows,
            prefix_rows=prefix_rows,
            span_dev=span_dev,
            heads_own=heads_own,
            kv_own=kv_own,
        ),
        (prefix_len, *packed, *decoded, held(proj), w_up),
        [SMEM] + [VMEM] * (2 * ten) + [VMEM, HBM],
        [
            out((half, width), F32),
            out((half, width), BF16),
            out(w_up.shape[1:], BF16),
        ],
        [pltpu.VMEM((ten * rows, heads_own * HD), F32), pltpu.SemaphoreType.DMA],
        limit=4,
    )
    (addends,), _, last_sent = halves_down(keep, send, "ten", ten)
    addends = [a for a, _ in addends]
    down, down_token = fetch(w_down, 0, last_sent)

    routed = call(
        functools.partial(
            route_kernel, parts=len(addends), groups=groups, local=local, rows=rows
        ),
        (
            *addends,
            hidden_in,
            norm_gain.reshape(1, width),
            router_w.T,
            expert_ids.T,
            down_token,
        ),
        [VMEM] * (len(addends) + 5),
        [out((rows, width), F32), out((rows, experts * SLOTS), F32)]
        + [out((local * SLOTS, width), BF16)] * groups,
        limit=3,
    )
    residual, weight_map, slots = routed[0], routed[1], routed[2:]

    block = [slots[0]] + [send_to(slots[d], "exp", d) for d in range(1, groups)]
    for bit in reversed(up_bits(ten)):
        block = block + [send_to(b, "ten", bit) for b in block]

    hidden_units = w_gate.shape[2]
    tile = min(512, hidden_units // 4)
    gate_first = hidden_units - tile
    gate_a, gate_token = fetch(w_gate, 0, slots[0], gate_first)
    gate_b, _ = fetch(w_gate, 0, gate_token, tile, gate_first)
    tiles = hidden_units // tile
    down_low_width = 2 * tile
    half = len(block) * SLOTS // 2
    returned = []
    for e in range(local):
        last, resident = e == local - 1, e == 0
        args, specs = [*block], [VMEM] * len(block)
        outs = [out((2 * half, hidden_units), BF16)]
        if resident:
            args += [held(gate_a), held(gate_b), held(up)]
            specs += [VMEM] * 3
        else:
            args += [held(next_low), held(gate_high), held(up_low), w_up, w_down]
            specs += [VMEM] * 3 + [HBM] * 2
            outs += [
                out((width, hidden_units - tile), BF16),
                out((hidden_units, down_low_width), BF16),
            ]
        if not last:
            args.append(w_gate)
            specs.append(HBM)
            outs.append(out((width, hidden_units - tile), BF16))
        hidden, *rest = call(
            functools.partial(
                hidden_kernel,
                pieces=len(block),
                expert=e,
                tile=tile,
                resident=resident,
                last=last,
            ),
            args,
            specs,
            outs,
            [
                pltpu.VMEM((2 * half, width), BF16),
                pltpu.VMEM((2 * half, hidden_units), F32),
                pltpu.SemaphoreType.DMA((tiles + 4,)),
            ],
            limit=3,
            flops=8 * half * width * hidden_units,
        )
        if not last:
            next_low = rest[-1]
        args, specs = [hidden], [VMEM]
        outs = [out((half, width), F32), out((half, width), BF16)]
        if resident:
            args.append(held(down))
            specs.append(VMEM)
        else:
            args += [held(rest[1]), w_down, rest[0], before]
            specs += [VMEM, HBM, VMEM, VMEM]
            outs.append(out((hidden_units, width - down_low_width), BF16))
        if not last:
            args += [w_gate, w_up]
            specs += [HBM, HBM]
            outs += [out((width, tile), BF16)] * 2
        keep, send, *rest = call(
            functools.partial(
                down_kernel, resident=resident, last=last, expert=e, tile=tile, extra=2
            ),
            args,
            specs,
            outs,
            [pltpu.SemaphoreType.DMA((2 + width // tile,))],
            limit=3,
            flops=4 * half * width * hidden_units,
        )
        if not last:
            gate_high, up_low = rest[-2:]
            rest = rest[:-2]
        cuts = 2 if groups > 2 else 1
        shares, share, before = halves_down(keep, send, "ten", ten, cuts)
        mine = [None] * groups
        each = groups // cuts
        for c in reversed(range(cuts)):
            addends = [a for a, _ in shares[c]]
            unused = rest if c == 0 else []
            pieces = call(
                functools.partial(
                    add_kernel,
                    parts=len(addends),
                    firsts=[first for _, first in shares[c]],
                    rows=share,
                    skip=len(unused),
                ),
                (*addends, *unused),
                [VMEM] * (len(addends) + len(unused)),
                [out((SLOTS, width), BF16)] * each,
                limit=3,
            )
            for i in reversed(range(each)):
                d = c * each + i
                mine[d] = send_to(pieces[i], "exp", d) if d else pieces[i]
        returned += mine
    return pl.pallas_call(
        functools.partial(mix_kernel, local=local, groups=groups),
        in_specs=[VMEM] * (2 + len(returned)),
        out_specs=VMEM,
        out_shape=jax.ShapeDtypeStruct((rows, width), BF16),
        compiler_params=pltpu.CompilerParams(vmem_limit_bytes=16 * MIB),
        name="mix",
    )(residual, weight_map, *returned)


def solution(mesh):
    in_specs = (
        P(("rep", "exp", "ten"), None),
        P(("rep", "exp", "ten"), None),
        P(None, ("rep", "exp", "ten"), None),
        P(None, ("rep", "exp"), "ten", None),
        P(None, ("rep", "exp", "ten"), None, None),
        P(("rep", "exp")),
        P(("rep", "exp", "ten")),
        P("ten", None),
        P(),
        P(),
        P(("rep", "exp", "ten"), None),
        P("exp", None, "ten"),
        P("exp", None, "ten"),
        P("exp", "ten", None),
    )
    out_specs = P(("rep", "exp", "ten"), None)

    return jax.shard_map(
        on_device, mesh=mesh, in_specs=in_specs, out_specs=out_specs, check_vma=False
    )
```
